256 devices in a mesh: grp: 32 (over z, x), dom: 8 (over y, core).
Axes of the slice: x: 4, y: 4, z: 8, core: 2. Of those that a mesh axis runs over, the one named last changes fastest.
Arguments:
- positions: float32 [3, 32768, 512], P(None, ('grp', 'dom')), may hold values from 0 to 1
- velocities: float32 [3, 32768, 512], P(None, ('grp', 'dom')), may hold values from -6 to 6
- masses: float32 [32768, 512], P(('grp', 'dom')), may hold values from 0.5 to 2
- block_halo: int32 [32768], P(('grp', 'dom')), may hold values from 0 to 32767, as said below
- block_shift: int32 [3, 32768], P(None, ('grp', 'dom')), may hold values from -1 to 1
- block_live: int32 [32768], P(('grp', 'dom')), may hold values from 64 to 512
- block_count: int32 [256], P(('grp', 'dom')), may hold values from 32 to 128
- home_slot: int32 [32768], replicated, may hold values from 0 to 32767, as said below
Outputs:
- halo_table: float32 [11, 32768], P(None, ('grp', 'dom'))
- kinetic: float32 [32768, 512], P(('grp', 'dom'))
- radial: float32 [32768, 512], P(('grp', 'dom'))
The draws below stay inside these ranges and needn't reach their ends.
Inputs may be any that keep to these rules, and one draw needn't show every extreme that they name: A permutation: the halo h is owned by the device of index home_slot[h] // 128 (grp+dom order), in its column home_slot[h] % 128. `block_halo`: the owner of a block's halo lies in the block's own index of grp or in the next one (index + 1, wrapping around); both occur.
All inputs are finite; a program needn't handle non-finite values.
Results may differ from the reference program's by a relative error of at most 0.0003.
Values sent between devices are 32-bit elements; how exact they have to be, the bound alone decides.
A program may use at most 64 MiB of HBM per device.

```python
import math
import jax
import jax.numpy as jnp
from jax import lax

BS = 512
BLK_DEV = 128
HALO_DEV = 128
NB = 32768
HALOS = 32768
N_GRP = 32
N_DOM = 8
DEVICES = 256


def owner_table(key):
    return jax.random.permutation(jax.random.fold_in(key, 11), HALOS).astype(jnp.int32)


def draw_home_slot(key, part):
    return owner_table(key)


def draw_block_halo(key, part):
    home = owner_table(key)
    inverse = jnp.argsort(home).astype(jnp.int32)
    window = N_DOM * HALO_DEV
    first_key, second_key, third_key = jax.random.split(jax.random.fold_in(key, 23), 3)
    limit = jax.random.randint(first_key, (NB,), 1, 2 * window + 1)
    picked = jax.random.randint(second_key, (NB,), 0, limit)
    mixing = jax.random.permutation(third_key, 2 * window).astype(jnp.int32)
    picked = mixing[picked]
    group_index = jnp.arange(NB, dtype=jnp.int32) // BLK_DEV // N_DOM
    column = (group_index + picked // window) % N_GRP * window + picked % window
    return inverse[column].astype(jnp.int32)


def touch_ends(values, rng, least, top_value):
    extent = values.shape
    spot = [jax.random.randint(jax.random.fold_in(rng, axis), (), 0, extent[axis]) for axis in range(len(extent))]
    values = values.at[tuple(spot)].set(least)
    longest = extent.index(max(extent))
    spot[longest] = (spot[longest] + 1) % extent[longest]
    return values.at[tuple(spot)].set(top_value)


def steps_of(rng, dims, cuts, smallest, top_value):
    level = 1.0
    for axis_at, shards_of in cuts:
        draws = jax.random.uniform(jax.random.fold_in(jax.random.fold_in(rng, 6), axis_at), (shards_of,), jnp.float32, smallest / len(cuts), top_value / len(cuts))
        level = level * jnp.repeat(jnp.exp(draws), dims[axis_at] // shards_of).reshape((-1,) + (1,) * (len(dims) - 1 - axis_at))
    return level


def normal_values(own_key, extent, scale, bound, pieces=(), kind=jnp.bfloat16):
    entries = scale * jax.random.normal(own_key, extent, jnp.float32)
    if pieces:
        entries = entries * steps_of(own_key, extent, pieces, -0.22, 0.18)
    return jnp.clip(entries, -bound, bound).astype(kind)


def setup_inputs(seed: int = 0) -> dict:
    key_of = jax.random.split(jax.random.key(seed), 9)
    positions = jnp.clip(1.0 * jax.random.uniform(key_of[0], (3, NB, BS), jnp.float32) ** steps_of(key_of[0], (3, NB, BS), ((1, 256),), -0.2, 0.2), 0.0, 1.0)
    velocities = normal_values(key_of[1], (3, NB, BS), 1.0, 6.0, ((1, 256),), jnp.float32)
    masses = jnp.clip(jnp.exp(math.log(2.0) - 1.3862944 * jax.random.uniform(key_of[2], (NB, BS), jnp.float32) ** steps_of(key_of[2], (NB, BS), ((0, 256),), -0.2, 0.2)), 0.5, 2.0)
    block_halo = draw_block_halo(jax.random.fold_in(key_of[8], 71), 0)
    block_shift = touch_ends(jax.random.randint(key_of[4], (3, NB), -1, 2), jax.random.fold_in(key_of[4], 1), -1, 1).astype(jnp.int32)
    block_live = touch_ends(jax.random.randint(key_of[5], (NB,), BS // 8, BS + 1), jax.random.fold_in(key_of[5], 1), BS // 8, BS).astype(jnp.int32)
    block_count = touch_ends(jax.random.randint(key_of[6], (DEVICES,), max(1, BLK_DEV // 4), BLK_DEV + 1), jax.random.fold_in(key_of[6], 1), max(1, BLK_DEV // 4), BLK_DEV).astype(jnp.int32)
    home_slot = draw_home_slot(jax.random.fold_in(key_of[8], 71), 0)
    return {"positions": positions, "velocities": velocities, "masses": masses, "block_halo": block_halo, "block_shift": block_shift, "block_live": block_live, "block_count": block_count, "home_slot": home_slot}


BOX = 1.0
EPSILON = 1e-6


def crossed(first, second):
    return jnp.stack([first[1] * second[2] - first[2] * second[1],
                      first[2] * second[0] - first[0] * second[2],
                      first[0] * second[1] - first[1] * second[0]])


def block_moments(positions, velocities, masses, block_shift, block_live, valid):
    lanes = jnp.arange(masses.shape[1], dtype=jnp.int32)
    live_mask = ((lanes[None, :] < block_live[:, None]) & valid[:, None]).astype(masses.dtype)
    weights = masses * live_mask
    unwrapped = positions + BOX * block_shift.astype(positions.dtype)[:, :, None]
    speed_sq = jnp.sum(velocities * velocities, axis=0)
    angular = crossed(unwrapped, velocities)
    rows = [jnp.sum(weights, axis=1)[None], jnp.sum(weights * unwrapped, axis=2),
            jnp.sum(weights * velocities, axis=2), jnp.sum(weights * speed_sq, axis=1)[None],
            jnp.sum(weights * angular, axis=2)]
    return jnp.concatenate(rows, axis=0), live_mask, unwrapped


def halo_properties(sums, total, halos):
    heavy = jnp.maximum(sums[0], 1.0)
    centre = sums[1:4] / heavy
    drift = sums[4:7] / heavy
    spread = sums[7] / heavy - jnp.sum(drift * drift, axis=0)
    spin = sums[8:11] / heavy - crossed(centre, drift)
    share = sums[0] * halos / total
    return jnp.concatenate([share[None], centre, drift, spread[None], spin], axis=0)


def particle_outputs(unwrapped, velocities, live_mask, stats):
    centre = stats[0:3][:, :, None]
    drift = stats[3:6][:, :, None]
    spread = stats[6][:, None]
    offset = velocities - drift
    kinetic = jnp.sum(offset * offset, axis=0) / (3.0 * spread + EPSILON)
    distance = unwrapped - centre
    radial = jnp.sum(distance * distance, axis=0)
    return kinetic * live_mask, radial * live_mask


def reference(positions, velocities, masses, block_halo, block_shift, block_live, block_count, home_slot):
    groups = block_count.shape[0]
    total_blocks = masses.shape[0]
    width = masses.shape[1]
    grouped_pos = positions.reshape(3, groups, BLK_DEV, width).transpose(1, 0, 2, 3)
    grouped_vel = velocities.reshape(3, groups, BLK_DEV, width).transpose(1, 0, 2, 3)
    grouped_mass = masses.reshape(groups, BLK_DEV, width)
    grouped_shift = block_shift.reshape(3, groups, BLK_DEV).transpose(1, 0, 2)
    grouped_live = block_live.reshape(groups, BLK_DEV)
    valid = jnp.arange(BLK_DEV, dtype=jnp.int32)[None, :] < block_count[:, None]

    def per_group(items):
        place, speed, weight, shift, alive, usable = items
        return block_moments(place, speed, weight, shift, alive, usable)[0]

    moments = lax.map(per_group, (grouped_pos, grouped_vel, grouped_mass, grouped_shift, grouped_live, valid))
    moments = moments.transpose(1, 0, 2).reshape(11, total_blocks)
    slots = home_slot[block_halo]
    halos = home_slot.shape[0]
    sums = jnp.zeros((11, halos), moments.dtype).at[:, slots].add(moments)
    total = jnp.sum(moments[0])
    halo_table = halo_properties(sums, total, halos)
    stats = halo_table[1:8][:, slots].reshape(7, groups, BLK_DEV).transpose(1, 0, 2)

    def outputs(items):
        place, speed, weight, shift, alive, usable, local_stats = items
        _, live_mask, unwrapped = block_moments(place, speed, weight, shift, alive, usable)
        return particle_outputs(unwrapped, speed, live_mask, local_stats)

    kinetic, radial = lax.map(outputs, (grouped_pos, grouped_vel, grouped_mass, grouped_shift, grouped_live, valid, stats))
    return halo_table, kinetic.reshape(total_blocks, width), radial.reshape(total_blocks, width)
```

```python
import functools

import jax
import jax.numpy as jnp
from jax import lax
from jax.experimental import pallas as pl
from jax.experimental.pallas import tpu as pltpu
from jax.sharding import PartitionSpec as P

MESH = pl.DeviceIdType.MESH
EPSILON = 1e-6
PLANE_GROUPS = 4
CHUNKS = 2
F32 = jnp.float32
NT = (((1,), (1,)), ((), ()))


def wrapped(index, size):
    return jnp.where(index >= size, index - size, index)


def iota(shape, dim):
    return lax.broadcasted_iota(jnp.int32, shape, dim)


def in_three(x):
    high = x.astype(jnp.bfloat16).astype(F32)
    rest = x - high
    middle = rest.astype(jnp.bfloat16).astype(F32)
    return jnp.concatenate([high, middle, rest - middle], axis=0)


def kernel(
    sizes,
    pos_hbm, vel_hbm, mass_hbm, halo_hbm, shift_hbm, live_hbm, count_hbm, slot_hbm,
    table_ref, kin_ref, rad_ref,
    pos, vel, mass, halo, shift, live, count, slots,
    live_bc, halo_bc, shift_bc, moments, extra, gather, plane, line,
    in_sem, small_sem, count_sem, send_sem, recv_sem,
):
    groups, domains, planes_groups = sizes
    blocks = mass.shape[0]
    width = mass.shape[1]
    depth = groups // planes_groups
    g, j = lax.axis_index("grp"), lax.axis_index("dom")
    z = g // planes_groups
    x = g - z * planes_groups
    nxt = wrapped(g + 1, groups)
    prv = jnp.where(g == 0, groups - 1, g - 1)

    order = sorted(range(domains), key=lambda k: -min(k, domains - k))
    near = [(grp, k, d) for grp, d in ((nxt, 0), (prv, 2)) for k in order]
    near += [(g, k, 1) for k in order if k]
    in_plane = [(a, k) for a in range(planes_groups) for k in range(domains) if (a, k) != (0, 0)]
    along = list(range(1, depth))

    def domain(k):
        return wrapped(j + k, domains)

    def plane_group(a):
        return z * planes_groups + wrapped(x + a, planes_groups)

    def line_group(a):
        return wrapped(z + a, depth) * planes_groups + x

    barrier = pltpu.get_barrier_semaphore()

    def greet(grp, dom):
        pl.semaphore_signal(barrier, inc=1, device_id=(grp, dom), device_id_type=MESH)

    for a in along:
        greet(line_group(a), j)
    for grp, k, _ in near:
        greet(grp, domain(k))
    for a, k in in_plane:
        greet(plane_group(a), domain(k))

    small = [
        pltpu.make_async_copy(live_hbm, live, small_sem.at[0]),
        pltpu.make_async_copy(halo_hbm, halo, small_sem.at[1]),
        pltpu.make_async_copy(shift_hbm, shift, small_sem.at[2]),
        pltpu.make_async_copy(slot_hbm, slots, small_sem.at[3]),
        pltpu.make_async_copy(count_hbm, count, count_sem),
    ]
    for copy in small[:3]:
        copy.start()
    small[4].start()
    part = blocks // CHUNKS
    big = []
    for c in range(CHUNKS):
        rows = pl.ds(c * part, part)
        big.append([
            pltpu.make_async_copy(mass_hbm.at[rows], mass.at[rows], in_sem.at[3 * c]),
            pltpu.make_async_copy(pos_hbm.at[:, rows], pos.at[:, rows], in_sem.at[3 * c + 1]),
            pltpu.make_async_copy(vel_hbm.at[:, rows], vel.at[:, rows], in_sem.at[3 * c + 2]),
        ])
        for copy in big[-1]:
            copy.start()
    small[3].start()
    for copy in small[:3]:
        copy.wait()
    small[4].wait()

    row = iota((1, blocks), 1)
    live_row = jnp.where(row < count[0], live[...], 0).astype(F32)
    halo_row = halo[...].astype(F32)
    shift_rows = shift[...].astype(F32)
    turned = jnp.concatenate(
        [live_row, halo_row, shift_rows, jnp.zeros((blocks - 5, blocks), F32)], axis=0
    ).T
    live_bc[...] = jnp.broadcast_to(turned[:, 0:1], (blocks, blocks))
    halo_bc[...] = jnp.broadcast_to(turned[:, 1:2], (blocks, blocks))
    for c in range(3):
        shift_bc[c] = jnp.broadcast_to(turned[:, 2 + c : 3 + c], (blocks, blocks))

    tiles = width // 128
    lane = iota((8, 128), 1)
    diagonal = lane - iota((8, 128), 0)

    def moment_step(i, sums):
        base = pl.multiple_of(i * 8, 8)
        rows = pl.ds(base, 8)
        alive = live_bc[rows, :]
        acc = None
        for t in range(tiles):
            cols = pl.ds(t * 128, 128)
            w = jnp.where((lane + t * 128).astype(F32) < alive, mass[rows, cols], 0.0)
            p = [pos[c, rows, cols] for c in range(3)]
            v = [vel[c, rows, cols] for c in range(3)]
            wv = [w * v[c] for c in range(3)]
            terms = [w] + [w * p[c] for c in range(3)] + wv
            terms.append(wv[0] * v[0] + wv[1] * v[1] + wv[2] * v[2])
            terms.append(p[1] * wv[2] - p[2] * wv[1])
            terms.append(p[2] * wv[0] - p[0] * wv[2])
            terms.append(p[0] * wv[1] - p[1] * wv[0])
            acc = terms if acc is None else [a + b for a, b in zip(acc, terms)]
        here = diagonal == base
        return tuple(
            s + jnp.where(here, jnp.sum(a, axis=1, keepdims=True), 0.0)
            for s, a in zip(sums, acc)
        )

    sums = tuple(jnp.zeros((8, 128), F32) for _ in range(11))
    for c in range(CHUNKS):
        for copy in big[c]:
            copy.wait()
        sums = lax.fori_loop(c * part // 8, (c + 1) * part // 8, moment_step, sums, unroll=4)
    m = [jnp.sum(s, axis=0, keepdims=True) for s in sums]
    s = [shift_rows[c : c + 1] for c in range(3)]
    raw_p, mom_v = m[1:4], m[4:7]
    ang = [
        m[8] + (s[1] * mom_v[2] - s[2] * mom_v[1]),
        m[9] + (s[2] * mom_v[0] - s[0] * mom_v[2]),
        m[10] + (s[0] * mom_v[1] - s[1] * mom_v[0]),
    ]
    place = [raw_p[c] + s[c] * m[0] for c in range(3)]

    small[3].wait()
    halo_int = halo[...]
    high_bits = halo_int // 128
    low_bits = halo_int - high_bits * 128
    table = slots[...]
    table_high = table // 256
    table_low = table - table_high * 256
    pick = jnp.where(iota((128, blocks), 0) == low_bits, 1.0, 0.0).astype(jnp.bfloat16)
    picked = jnp.dot(
        jnp.concatenate([table_high, table_low], axis=0).astype(F32).astype(jnp.bfloat16),
        pick,
        preferred_element_type=F32,
    )
    long = table.shape[0]
    both = picked[:long] * 256.0 + picked[long:]
    slot_row = jnp.sum(
        jnp.where(iota((long, blocks), 0) == high_bits, both, 0.0), axis=0, keepdims=True
    )

    message = jnp.concatenate(
        [m[0], *place, *mom_v, m[7], halo_row, slot_row, *ang, jnp.zeros((3, blocks), F32)], axis=0
    )
    moments[...] = message
    extra[...] = m[0]
    me = x * domains + j
    gather[pl.ds(domains + j, 1)] = message[None]
    plane[pl.ds(me, 1)] = m[0][None]

    pl.semaphore_wait(barrier, len(near) + len(in_plane) + len(along))

    for a, k in in_plane:
        pltpu.make_async_remote_copy(
            extra, plane.at[me], send_sem.at[0], recv_sem.at[3],
            device_id=(plane_group(a), domain(k)), device_id_type=MESH,
        ).start()
    for grp, k, d in near:
        pltpu.make_async_remote_copy(
            moments, gather.at[d * domains + j], send_sem.at[1], recv_sem.at[d],
            device_id=(grp, domain(k)), device_id_type=MESH,
        ).start()

    def arrived(d):
        n = domains - 1 if d == 1 else domains
        span = gather.at[pl.ds(d * domains, n)]
        pltpu.make_async_copy(span, span, recv_sem.at[d]).wait()

    def hot(d, base_bc, at):
        return jnp.concatenate(
            [
                jnp.where(base_bc == gather[d * domains + k, at : at + 1, :], 1.0, 0.0).astype(jnp.bfloat16)
                for k in range(domains)
            ],
            axis=1,
        )

    def parts(d, row0, rows):
        values = [
            in_three(gather[d * domains + k, row0 : row0 + rows, :]).astype(jnp.bfloat16)
            for k in range(domains)
        ]
        return jnp.concatenate(values, axis=1)

    def summed(d):
        return lax.dot_general(
            hot(d, halo_bc[...], 8), parts(d, 0, 8), NT, preferred_element_type=F32
        )

    def owned(d):
        mine = (iota((blocks, blocks), 0) + (g * domains + j) * blocks).astype(F32)
        return lax.dot_general(
            hot(d, mine, 9), parts(d, 0, 16), NT, preferred_element_type=F32
        )

    arrived(1)
    stats = summed(1)
    table_sums = owned(1)

    n_plane = len(in_plane)
    pltpu.make_async_copy(plane.at[pl.ds(0, n_plane)], plane.at[pl.ds(0, n_plane)], recv_sem.at[3]).wait()
    plane_mass = jnp.sum(plane[...], axis=0)
    extra_line = plane_mass
    pltpu.make_async_copy(plane.at[pl.ds(0, n_plane)], plane.at[pl.ds(0, n_plane)], send_sem.at[0]).wait()
    extra[...] = extra_line
    line[pl.ds(z, 1)] = plane_mass[None]
    for a in along:
        pltpu.make_async_remote_copy(
            extra, line.at[z], send_sem.at[2], recv_sem.at[4],
            device_id=(line_group(a), j), device_id_type=MESH,
        ).start()

    arrived(0)
    arrived(2)
    stats = stats + summed(0) + summed(2)
    stats = stats[:, 0:8] + stats[:, 8:16] + stats[:, 16:24]
    wide = [jnp.broadcast_to(stats[:, k : k + 1], (blocks, 128)) for k in range(8)]
    heavy = 1.0 / jnp.maximum(wide[0], 1.0)
    drift = [wide[4 + c] * heavy for c in range(3)]
    spread = wide[7] * heavy - (drift[0] * drift[0] + drift[1] * drift[1] + drift[2] * drift[2])
    over = 1.0 / (3.0 * spread + EPSILON)
    centre = [wide[1 + c] * heavy - shift_bc[c] for c in range(3)]

    for i in range(blocks // 8):
        r = slice(8 * i, 8 * i + 8)
        alive = live_bc[r, :]
        for t in range(tiles):
            q = slice(128 * t, 128 * t + 128)
            mask = (lane + t * 128).astype(F32) < alive
            dv = [vel[c, r, q] - drift[c][r] for c in range(3)]
            dp = [pos[c, r, q] - centre[c][r] for c in range(3)]
            kin = (dv[0] * dv[0] + dv[1] * dv[1] + dv[2] * dv[2]) * over[r]
            rad = dp[0] * dp[0] + dp[1] * dp[1] + dp[2] * dp[2]
            kin_ref[r, q] = jnp.where(mask, kin, 0.0)
            rad_ref[r, q] = jnp.where(mask, rad, 0.0)

    table_sums = table_sums + owned(0)
    own = jnp.concatenate([table_sums, jnp.zeros((blocks, 128 - 48), F32)], axis=1).T
    own = own[0:16] + own[16:32] + own[32:48]
    heavy = jnp.maximum(own[0:1], 1.0)
    c = [own[1 + i : 2 + i] / heavy for i in range(3)]
    d = [own[4 + i : 5 + i] / heavy for i in range(3)]
    spread = own[7:8] / heavy - (d[0] * d[0] + d[1] * d[1] + d[2] * d[2])
    spin = [
        own[10:11] / heavy - (c[1] * d[2] - c[2] * d[1]),
        own[11:12] / heavy - (c[2] * d[0] - c[0] * d[2]),
        own[12:13] / heavy - (c[0] * d[1] - c[1] * d[0]),
    ]

    n_line = len(along)
    pltpu.make_async_copy(line.at[pl.ds(0, n_line)], line.at[pl.ds(0, n_line)], recv_sem.at[4]).wait()
    total = jnp.sum(jnp.sum(line[...], axis=0), axis=1, keepdims=True)
    share = own[0:1] * float(groups * domains * blocks) / total
    table_ref[...] = jnp.concatenate([share, *c, *d, spread, *spin], axis=0)

    pltpu.make_async_copy(line.at[pl.ds(0, n_line)], line.at[pl.ds(0, n_line)], send_sem.at[2]).wait()
    n_near = len(near)
    pltpu.make_async_copy(gather.at[pl.ds(0, n_near)], gather.at[pl.ds(0, n_near)], send_sem.at[1]).wait()


def solution(mesh, plane_groups=PLANE_GROUPS):
    groups, domains = mesh.shape["grp"], mesh.shape["dom"]
    both = ("grp", "dom")

    def local(positions, velocities, masses, block_halo, block_shift, block_live, block_count, home_slot):
        blocks, width = masses.shape
        hbm = pl.BlockSpec(memory_space=pltpu.HBM)
        vmem = pl.BlockSpec(memory_space=pltpu.VMEM)
        long = home_slot.shape[0] // 128
        return pl.pallas_call(
            functools.partial(kernel, (groups, domains, plane_groups)),
            out_shape=(
                jax.ShapeDtypeStruct((11, blocks), F32),
                jax.ShapeDtypeStruct((blocks, width), F32),
                jax.ShapeDtypeStruct((blocks, width), F32),
            ),
            in_specs=[hbm] * 8,
            out_specs=(vmem, vmem, vmem),
            scratch_shapes=[
                pltpu.VMEM((3, blocks, width), F32),
                pltpu.VMEM((3, blocks, width), F32),
                pltpu.VMEM((blocks, width), F32),
                pltpu.VMEM((1, blocks), jnp.int32),
                pltpu.VMEM((3, blocks), jnp.int32),
                pltpu.VMEM((1, blocks), jnp.int32),
                pltpu.SMEM((1,), jnp.int32),
                pltpu.VMEM((long, 128), jnp.int32),
                pltpu.VMEM((blocks, blocks), F32),
                pltpu.VMEM((blocks, blocks), F32),
                pltpu.VMEM((3, blocks, blocks), F32),
                pltpu.VMEM((16, blocks), F32),
                pltpu.VMEM((1, blocks), F32),
                pltpu.VMEM((3 * domains, 16, blocks), F32),
                pltpu.VMEM((plane_groups * domains, 1, blocks), F32),
                pltpu.VMEM((groups // plane_groups, 1, blocks), F32),
                pltpu.SemaphoreType.DMA((3 * CHUNKS,)),
                pltpu.SemaphoreType.DMA((4,)),
                pltpu.SemaphoreType.DMA,
                pltpu.SemaphoreType.DMA((3,)),
                pltpu.SemaphoreType.DMA((5,)),
            ],
            compiler_params=pltpu.CompilerParams(collective_id=0, has_side_effects=True),
        )(
            positions, velocities, masses,
            block_halo.reshape(1, blocks), block_shift, block_live.reshape(1, blocks), block_count,
            home_slot.reshape(long, 128),
        )

    return jax.shard_map(
        local,
        mesh=mesh,
        in_specs=(
            P(None, both, None), P(None, both, None), P(both, None), P(both), P(None, both), P(both), P(both), P(),
        ),
        out_specs=(P(None, both), P(both, None), P(both, None)),
        check_vma=False,
    )
```

```python
import functools

import jax
import jax.numpy as jnp
from jax import lax
from jax.experimental import pallas as pl
from jax.experimental.pallas import tpu as pltpu
from jax.sharding import PartitionSpec as P

MESH = pl.DeviceIdType.MESH
EPSILON = 1e-6
PLANE_GROUPS = 4
ROOT_PLANES = 2
CHUNKS = 2
F32 = jnp.float32
NT = (((1,), (1,)), ((), ()))


def wrapped(index, size):
    return jnp.where(index >= size, index - size, index)


def iota(shape, dim):
    return lax.broadcasted_iota(jnp.int32, shape, dim)


def in_three(x):
    high = x.astype(jnp.bfloat16).astype(F32)
    rest = x - high
    middle = rest.astype(jnp.bfloat16).astype(F32)
    return jnp.concatenate([high, middle, rest - middle], axis=0)


def kernel(
    sizes,
    pos_hbm, vel_hbm, mass_hbm, halo_hbm, shift_hbm, live_hbm, count_hbm, slot_hbm,
    table_ref, kin_ref, rad_ref,
    pos, vel, mass, halo, shift, live, count, slots,
    live_bc, halo_bc, shift_bc, moments, extra, gather, masses, line,
    in_sem, small_sem, count_sem, send_sem, recv_sem,
):
    groups, domains, planes_groups = sizes
    blocks = mass.shape[0]
    width = mass.shape[1]
    depth = groups // planes_groups
    g, j = lax.axis_index("grp"), lax.axis_index("dom")
    z = g // planes_groups
    x = g - z * planes_groups
    nxt = wrapped(g + 1, groups)
    prv = jnp.where(g == 0, groups - 1, g - 1)

    order = sorted(range(domains), key=lambda k: -min(k, domains - k))
    near = [(grp, k, d) for grp, d in ((nxt, 0), (prv, 2)) for k in order]
    near += [(g, k, 1) for k in order if k]
    roots = min(ROOT_PLANES, depth - 1)
    plane = planes_groups * domains
    everyone = groups * domains
    me = g * domains + j
    is_root = z < roots

    def domain(k):
        return wrapped(j + k, domains)

    def greet(grp, dom):
        pl.semaphore_signal(barrier, inc=1, device_id=(grp, dom), device_id_type=MESH)

    small = [
        pltpu.make_async_copy(live_hbm, live, small_sem.at[0]),
        pltpu.make_async_copy(count_hbm, count, count_sem),
        pltpu.make_async_copy(halo_hbm, halo, small_sem.at[1]),
        pltpu.make_async_copy(shift_hbm, shift, small_sem.at[2]),
        pltpu.make_async_copy(slot_hbm, slots, small_sem.at[3]),
    ]
    for copy in small:
        copy.start()
    part = blocks // CHUNKS
    big = []
    for c in range(CHUNKS):
        rows = pl.ds(c * part, part)
        big.append([
            pltpu.make_async_copy(mass_hbm.at[rows], mass.at[rows], in_sem.at[3 * c]),
            pltpu.make_async_copy(pos_hbm.at[:, rows], pos.at[:, rows], in_sem.at[3 * c + 1]),
            pltpu.make_async_copy(vel_hbm.at[:, rows], vel.at[:, rows], in_sem.at[3 * c + 2]),
        ])
        for copy in big[-1]:
            copy.start()

    barrier = pltpu.get_barrier_semaphore()
    for grp, k, _ in near:
        greet(grp, domain(k))

    @pl.when(is_root)
    def _():
        @pl.loop(0, groups)
        def _(step):
            grp = groups - 1 - step
            for dom in range(domains):
                @pl.when((grp != g) | (dom != j))
                def _():
                    greet(grp, dom)

    for copy in small:
        copy.wait()

    row = iota((1, blocks), 1)
    live_row = jnp.where(row < count[...], live[...], 0).astype(F32)
    halo_row = halo[...].astype(F32)
    shift_rows = shift[...].astype(F32)
    turned = jnp.concatenate(
        [live_row, halo_row, shift_rows, jnp.zeros((blocks - 5, blocks), F32)], axis=0
    ).T
    live_bc[...] = jnp.broadcast_to(turned[:, 0:1], (blocks, blocks))

    halo_int = halo[...]
    high_bits = halo_int // 128
    low_bits = halo_int - high_bits * 128
    table = slots[...]
    table_high = table // 256
    table_low = table - table_high * 256
    pick = jnp.where(iota((128, blocks), 0) == low_bits, 1.0, 0.0).astype(jnp.bfloat16)
    picked = jnp.dot(
        jnp.concatenate([table_high, table_low], axis=0).astype(F32).astype(jnp.bfloat16),
        pick,
        preferred_element_type=F32,
    )
    long = table.shape[0]
    both = picked[:long] * 256.0 + picked[long:]
    slot_row = jnp.sum(
        jnp.where(iota((long, blocks), 0) == high_bits, both, 0.0), axis=0, keepdims=True
    )

    tiles = width // 128
    lane = iota((8, 128), 1)
    diagonal = lane - iota((8, 128), 0)

    def moment_step(i, sums):
        base = pl.multiple_of(i * 8, 8)
        rows = pl.ds(base, 8)
        alive = live_bc[rows, :]
        acc = None
        for t in range(tiles):
            cols = pl.ds(t * 128, 128)
            w = jnp.where((lane + t * 128).astype(F32) < alive, mass[rows, cols], 0.0)
            p = [pos[c, rows, cols] for c in range(3)]
            v = [vel[c, rows, cols] for c in range(3)]
            wv = [w * v[c] for c in range(3)]
            terms = [w] + [w * p[c] for c in range(3)] + wv
            terms.append(wv[0] * v[0] + wv[1] * v[1] + wv[2] * v[2])
            terms.append(p[1] * wv[2] - p[2] * wv[1])
            terms.append(p[2] * wv[0] - p[0] * wv[2])
            terms.append(p[0] * wv[1] - p[1] * wv[0])
            acc = terms if acc is None else [a + b for a, b in zip(acc, terms)]
        here = diagonal == base
        return tuple(
            s + jnp.where(here, jnp.sum(a, axis=1, keepdims=True), 0.0)
            for s, a in zip(sums, acc)
        )

    sums = tuple(jnp.zeros((8, 128), F32) for _ in range(11))
    for c in range(CHUNKS):
        for copy in big[c]:
            copy.wait()
        sums = lax.fori_loop(c * part // 8, (c + 1) * part // 8, moment_step, sums, unroll=4)
    m = [jnp.sum(s, axis=0, keepdims=True) for s in sums]
    s = [shift_rows[c : c + 1] for c in range(3)]
    raw_p, mom_v = m[1:4], m[4:7]
    ang = [
        m[8] + (s[1] * mom_v[2] - s[2] * mom_v[1]),
        m[9] + (s[2] * mom_v[0] - s[0] * mom_v[2]),
        m[10] + (s[0] * mom_v[1] - s[1] * mom_v[0]),
    ]
    place = [raw_p[c] + s[c] * m[0] for c in range(3)]

    message = jnp.concatenate(
        [m[0], *place, *mom_v, m[7], halo_row, slot_row, *ang, jnp.zeros((3, blocks), F32)], axis=0
    )
    moments[...] = message
    extra[...] = m[0]
    gather[pl.ds(domains + j, 1)] = message[None]
    masses[pl.ds(me, 1)] = m[0][None]

    pl.semaphore_wait(barrier, jnp.where(is_root, len(near) + roots * plane - 1, len(near) + roots * plane))

    def send_mass(grp, dom):
        pltpu.make_async_remote_copy(
            extra, masses.at[me], send_sem.at[0], recv_sem.at[3],
            device_id=(grp, dom), device_id_type=MESH,
        ).start()

    for r in range(roots):
        for a in range(planes_groups):
            for k in order:
                grp = r * planes_groups + wrapped(x + a, planes_groups)
                if (a, k) == (0, 0):
                    @pl.when(z != r)
                    def _():
                        send_mass(grp, j)
                else:
                    send_mass(grp, domain(k))
    for grp, k, d in near:
        pltpu.make_async_remote_copy(
            moments, gather.at[d * domains + j], send_sem.at[1], recv_sem.at[d],
            device_id=(grp, domain(k)), device_id_type=MESH,
        ).start()
    halo_bc[...] = jnp.broadcast_to(turned[:, 1:2], (blocks, blocks))
    for c in range(3):
        shift_bc[c] = jnp.broadcast_to(turned[:, 2 + c : 3 + c], (blocks, blocks))

    def arrived(d):
        n = domains - 1 if d == 1 else domains
        span = gather.at[pl.ds(d * domains, n)]
        pltpu.make_async_copy(span, span, recv_sem.at[d]).wait()

    def hot(d, base_bc, at):
        return jnp.concatenate(
            [
                jnp.where(base_bc == gather[d * domains + k, at : at + 1, :], 1.0, 0.0).astype(jnp.bfloat16)
                for k in range(domains)
            ],
            axis=1,
        )

    def parts(d, row0, rows):
        values = [
            in_three(gather[d * domains + k, row0 : row0 + rows, :]).astype(jnp.bfloat16)
            for k in range(domains)
        ]
        return jnp.concatenate(values, axis=1)

    def summed(d):
        return lax.dot_general(
            hot(d, halo_bc[...], 8), parts(d, 0, 8), NT, preferred_element_type=F32
        )

    def owned(d):
        mine = (iota((blocks, blocks), 0) + (g * domains + j) * blocks).astype(F32)
        return lax.dot_general(
            parts(d, 0, 16), hot(d, mine, 9), NT, preferred_element_type=F32
        )

    arrived(1)
    stats = summed(1)
    table_sums = owned(1)

    arrived(2)
    stats = stats + summed(2)
    arrived(0)
    stats = stats + summed(0)
    stats = stats[:, 0:8] + stats[:, 8:16] + stats[:, 16:24]
    wide = [jnp.broadcast_to(stats[:, k : k + 1], (blocks, 128)) for k in range(8)]
    heavy = 1.0 / jnp.maximum(wide[0], 1.0)
    drift = [wide[4 + c] * heavy for c in range(3)]
    spread = wide[7] * heavy - (drift[0] * drift[0] + drift[1] * drift[1] + drift[2] * drift[2])
    over = 1.0 / (3.0 * spread + EPSILON)
    centre = [wide[1 + c] * heavy - shift_bc[c] for c in range(3)]

    for i in range(blocks // 8):
        r = slice(8 * i, 8 * i + 8)
        alive = live_bc[r, :]
        for t in range(tiles):
            q = slice(128 * t, 128 * t + 128)
            mask = (lane + t * 128).astype(F32) < alive
            dv = [vel[c, r, q] - drift[c][r] for c in range(3)]
            dp = [pos[c, r, q] - centre[c][r] for c in range(3)]
            kin = (dv[0] * dv[0] + dv[1] * dv[1] + dv[2] * dv[2]) * over[r]
            rad = dp[0] * dp[0] + dp[1] * dp[1] + dp[2] * dp[2]
            kin_ref[r, q] = jnp.where(mask, kin, 0.0)
            rad_ref[r, q] = jnp.where(mask, rad, 0.0)

    table_sums = table_sums + owned(0)
    own = table_sums[0:16] + table_sums[16:32] + table_sums[32:48]
    heavy = jnp.maximum(own[0:1], 1.0)
    c = [own[1 + i : 2 + i] / heavy for i in range(3)]
    d = [own[4 + i : 5 + i] / heavy for i in range(3)]
    spread = own[7:8] / heavy - (d[0] * d[0] + d[1] * d[1] + d[2] * d[2])
    spin = [
        own[10:11] / heavy - (c[1] * d[2] - c[2] * d[1]),
        own[11:12] / heavy - (c[2] * d[0] - c[0] * d[2]),
        own[12:13] / heavy - (c[0] * d[1] - c[1] * d[0]),
    ]

    def along(r):
        return [t for t in range(roots, depth) if (t > depth // 2) == (r == 0)] if roots > 1 else list(range(roots, depth))

    def tell(t):
        return pltpu.make_async_remote_copy(
            line, line, send_sem.at[2], recv_sem.at[4],
            device_id=(t * planes_groups + x, j), device_id_type=MESH,
        )

    @pl.when(is_root)
    def _():
        others = masses.at[pl.ds(0, everyone - 1)]
        pltpu.make_async_copy(others, others, recv_sem.at[3]).wait()
        line[...] = jnp.sum(masses[...], axis=0)
        for r in (0, roots - 1)[: min(roots, 2)]:
            @pl.when(z == r)
            def _():
                for t in along(r):
                    tell(t).start()

    @pl.when(z >= roots)
    def _():
        pltpu.make_async_copy(line, line, recv_sem.at[4]).wait()

    total = jnp.sum(line[...], axis=1, keepdims=True)
    share = own[0:1] * float(groups * domains * blocks) / total
    table_ref[...] = jnp.concatenate([share, *c, *d, spread, *spin], axis=0)

    for r in (0, roots - 1)[: min(roots, 2)]:
        @pl.when(z == r)
        def _():
            told = masses.at[pl.ds(0, len(along(r)))]
            pltpu.make_async_copy(told, told, send_sem.at[2]).wait()

    n_mass = roots * plane

    @pl.when(is_root)
    def _():
        sent = masses.at[pl.ds(0, n_mass - 1)]
        pltpu.make_async_copy(sent, sent, send_sem.at[0]).wait()

    @pl.when(z >= roots)
    def _():
        sent = masses.at[pl.ds(0, n_mass)]
        pltpu.make_async_copy(sent, sent, send_sem.at[0]).wait()

    n_near = len(near)
    pltpu.make_async_copy(gather.at[pl.ds(0, n_near)], gather.at[pl.ds(0, n_near)], send_sem.at[1]).wait()


def flush(table_ref, kin_ref, rad_ref, table_hbm, kin_hbm, rad_hbm, sem):
    pairs = ((kin_ref, kin_hbm), (rad_ref, rad_hbm), (table_ref, table_hbm))
    copies = [pltpu.make_async_copy(a, b, sem.at[i]) for i, (a, b) in enumerate(pairs)]
    for copy in copies:
        copy.start()
    for copy in copies:
        copy.wait()


def solution(mesh, plane_groups=PLANE_GROUPS):
    groups, domains = mesh.shape["grp"], mesh.shape["dom"]
    both = ("grp", "dom")

    def local(positions, velocities, masses, block_halo, block_shift, block_live, block_count, home_slot):
        blocks, width = masses.shape
        hbm = pl.BlockSpec(memory_space=pltpu.HBM)
        vmem = pl.BlockSpec(memory_space=pltpu.VMEM)
        long = home_slot.shape[0] // 128
        results = pl.pallas_call(
            functools.partial(kernel, (groups, domains, plane_groups)),
            out_shape=(
                pltpu.VMEM((11, blocks), F32),
                pltpu.VMEM((blocks, width), F32),
                pltpu.VMEM((blocks, width), F32),
            ),
            in_specs=[hbm] * 8,
            out_specs=(vmem, vmem, vmem),
            scratch_shapes=[
                pltpu.VMEM((3, blocks, width), F32),
                pltpu.VMEM((3, blocks, width), F32),
                pltpu.VMEM((blocks, width), F32),
                pltpu.VMEM((1, blocks), jnp.int32),
                pltpu.VMEM((3, blocks), jnp.int32),
                pltpu.VMEM((1, blocks), jnp.int32),
                pltpu.VMEM((1, 1), jnp.int32),
                pltpu.VMEM((long, 128), jnp.int32),
                pltpu.VMEM((blocks, blocks), F32),
                pltpu.VMEM((blocks, blocks), F32),
                pltpu.VMEM((3, blocks, blocks), F32),
                pltpu.VMEM((16, blocks), F32),
                pltpu.VMEM((1, blocks), F32),
                pltpu.VMEM((3 * domains, 16, blocks), F32),
                pltpu.VMEM((groups * domains, 1, blocks), F32),
                pltpu.VMEM((1, blocks), F32),
                pltpu.SemaphoreType.DMA((3 * CHUNKS,)),
                pltpu.SemaphoreType.DMA((4,)),
                pltpu.SemaphoreType.DMA,
                pltpu.SemaphoreType.DMA((3,)),
                pltpu.SemaphoreType.DMA((5,)),
            ],
            compiler_params=pltpu.CompilerParams(collective_id=0, has_side_effects=True),
        )(
            positions, velocities, masses,
            block_halo.reshape(1, blocks), block_shift, block_live.reshape(1, blocks), block_count.reshape(1, 1),
            home_slot.reshape(long, 128),
        )
        return pl.pallas_call(
            flush,
            out_shape=tuple(jax.ShapeDtypeStruct(r.shape, F32) for r in results),
            in_specs=[vmem] * 3,
            out_specs=(hbm,) * 3,
            scratch_shapes=[pltpu.SemaphoreType.DMA((3,))],
        )(*[pltpu.with_memory_space_constraint(r, pltpu.VMEM) for r in results])

    return jax.shard_map(
        local,
        mesh=mesh,
        in_specs=(
            P(None, both, None), P(None, both, None), P(both, None), P(both), P(None, both), P(both), P(both), P(),
        ),
        out_specs=(P(None, both), P(both, None), P(both, None)),
        check_vma=False,
    )
```

```python
import functools

import jax
import jax.numpy as jnp
from jax import lax
from jax.experimental import pallas as pl
from jax.experimental.pallas import tpu as pltpu
from jax.sharding import PartitionSpec as P

MESH = pl.DeviceIdType.MESH
EPSILON = 1e-6
PLANE_GROUPS = 4
ROOT = 1
CHUNKS = 4
F32 = jnp.float32
NT = (((1,), (1,)), ((), ()))


def wrapped(index, size):
    return jnp.where(index >= size, index - size, index)


def iota(shape, dim):
    return lax.broadcasted_iota(jnp.int32, shape, dim)


def in_three(x):
    high = x.astype(jnp.bfloat16).astype(F32)
    rest = x - high
    middle = rest.astype(jnp.bfloat16).astype(F32)
    return jnp.concatenate([high, middle, rest - middle], axis=0)


def kernel(
    sizes,
    pos_hbm, vel_hbm, mass_hbm, halo_hbm, shift_hbm, live_hbm, count_hbm, slot_hbm,
    table_ref, kin_ref, rad_ref,
    pos, vel, mass, halo, shift, live, count, slots,
    live_bc, halo_bc, shift_bc, moments, rest, gather, gather_rest, masses, line,
    in_sem, small_sem, count_sem, send_sem, recv_sem,
):
    groups, domains, planes_groups = sizes
    blocks = mass.shape[0]
    width = mass.shape[1]
    depth = groups // planes_groups
    g, j = lax.axis_index("grp"), lax.axis_index("dom")
    z = g // planes_groups
    x = g - z * planes_groups
    nxt = wrapped(g + 1, groups)
    prv = jnp.where(g == 0, groups - 1, g - 1)

    order = sorted(range(domains), key=lambda k: -min(k, domains - k))
    near = [(nxt, k, 0) for k in order] + [(prv, k, 2) for k in order] + [(g, k, 1) for k in order if k]
    me = g * domains + j
    roots = depth // 2
    everyone = groups * domains
    is_root = (z < roots) & (x == 0) & (j == ROOT)

    def domain(k):
        return wrapped(j + k, domains)

    def greet(grp, dom):
        pl.semaphore_signal(barrier, inc=1, device_id=(grp, dom), device_id_type=MESH)

    small = [
        pltpu.make_async_copy(live_hbm, live, small_sem.at[0]),
        pltpu.make_async_copy(count_hbm, count, count_sem),
        pltpu.make_async_copy(halo_hbm, halo, small_sem.at[1]),
        pltpu.make_async_copy(shift_hbm, shift, small_sem.at[2]),
        pltpu.make_async_copy(slot_hbm, slots, small_sem.at[3]),
    ]
    for copy in small[:2]:
        copy.start()
    part = blocks // CHUNKS
    big = []
    for c in range(CHUNKS):
        rows = pl.ds(c * part, part)
        big.append([
            pltpu.make_async_copy(mass_hbm.at[rows], mass.at[rows], in_sem.at[3 * c]),
            pltpu.make_async_copy(pos_hbm.at[:, rows], pos.at[:, rows], in_sem.at[3 * c + 1]),
            pltpu.make_async_copy(vel_hbm.at[:, rows], vel.at[:, rows], in_sem.at[3 * c + 2]),
        ])
        for copy in big[-1]:
            copy.start()

    for copy in small[2:]:
        copy.start()
    barrier = pltpu.get_barrier_semaphore()
    for grp, k, _ in near:
        greet(grp, domain(k))

    @pl.when(is_root)
    def _():
        @pl.loop(0, depth)
        def _(step):
            there = depth - 1 - step
            for a in range(planes_groups):
                for k in range(domains):
                    if (a, k) != (0, ROOT):
                        greet(there * planes_groups + a, k)

            @pl.when(there != z)
            def _():
                greet(there * planes_groups, ROOT)

    for copy in small[:2]:
        copy.wait()

    row = iota((1, blocks), 1)
    live_row = jnp.where(row < count[...], live[...], 0).astype(F32)
    live_bc[...] = jnp.broadcast_to(live_row, (blocks, blocks)).T

    tiles = width // 128
    lane = iota((8, 128), 1)
    diagonal = lane - iota((8, 128), 0)

    def moment_step(i, sums):
        base = pl.multiple_of(i * 8, 8)
        rows = pl.ds(base, 8)
        alive = live_bc[rows, :]
        acc = None
        for t in range(tiles):
            cols = pl.ds(t * 128, 128)
            w = jnp.where((lane + t * 128).astype(F32) < alive, mass[rows, cols], 0.0)
            p = [pos[c, rows, cols] for c in range(3)]
            v = [vel[c, rows, cols] for c in range(3)]
            wv = [w * v[c] for c in range(3)]
            terms = [w] + [w * p[c] for c in range(3)] + wv
            terms.append(wv[0] * v[0] + wv[1] * v[1] + wv[2] * v[2])
            terms.append(p[1] * wv[2] - p[2] * wv[1])
            terms.append(p[2] * wv[0] - p[0] * wv[2])
            terms.append(p[0] * wv[1] - p[1] * wv[0])
            acc = terms if acc is None else [a + b for a, b in zip(acc, terms)]
        here = diagonal == base
        return tuple(
            s + jnp.where(here, jnp.sum(a, axis=1, keepdims=True), 0.0)
            for s, a in zip(sums, acc)
        )

    sums = tuple(jnp.zeros((8, 128), F32) for _ in range(11))
    for c in range(CHUNKS):
        for copy in big[c]:
            copy.wait()
        sums = lax.fori_loop(c * part // 8, (c + 1) * part // 8, moment_step, sums, unroll=4)
    for copy in small[2:]:
        copy.wait()
    halo_row = halo[...].astype(F32)
    shift_rows = shift[...].astype(F32)
    m = [jnp.sum(s, axis=0, keepdims=True) for s in sums]
    s = [shift_rows[c : c + 1] for c in range(3)]
    raw_p, mom_v = m[1:4], m[4:7]
    ang = [
        m[8] + (s[1] * mom_v[2] - s[2] * mom_v[1]),
        m[9] + (s[2] * mom_v[0] - s[0] * mom_v[2]),
        m[10] + (s[0] * mom_v[1] - s[1] * mom_v[0]),
    ]
    place = [raw_p[c] + s[c] * m[0] for c in range(3)]

    moments[0:9, :] = jnp.concatenate([m[0], *place, *mom_v, m[7], halo_row], axis=0)
    gather[domains + j, 0:9, :] = moments[0:9, :]
    masses[pl.ds(me, 1), :] = m[0]

    pl.semaphore_wait(barrier, jnp.where(is_root, len(near) + roots - 1, len(near) + roots))

    for r in range(roots):
        @pl.when(jnp.logical_not(is_root & (z == r)))
        def _():
            pltpu.make_async_remote_copy(
                moments.at[pl.ds(0, 1)], masses.at[pl.ds(me, 1)], send_sem.at[0], recv_sem.at[3],
                device_id=(r * planes_groups, ROOT), device_id_type=MESH,
            ).start()

    for grp, k, d in near:
        pltpu.make_async_remote_copy(
            moments.at[pl.ds(0, 9)], gather.at[d * domains + j, pl.ds(0, 9)], send_sem.at[1], recv_sem.at[d],
            device_id=(grp, domain(k)), device_id_type=MESH,
        ).start()
    halo_int = halo[...]
    high_bits = halo_int // 128
    low_bits = halo_int - high_bits * 128
    table = slots[...]
    table_high = table // 256
    table_low = table - table_high * 256
    pick = jnp.where(iota((128, blocks), 0) == low_bits, 1.0, 0.0).astype(jnp.bfloat16)
    picked = jnp.dot(
        jnp.concatenate([table_high, table_low], axis=0).astype(F32).astype(jnp.bfloat16),
        pick,
        preferred_element_type=F32,
    )
    long = table.shape[0]
    both = picked[:long] * 256.0 + picked[long:]
    slot_row = jnp.sum(
        jnp.where(iota((long, blocks), 0) == high_bits, both, 0.0), axis=0, keepdims=True
    )

    rest[0:4, :] = jnp.concatenate([slot_row, *ang], axis=0)
    gather_rest[domains + j, 0:4, :] = rest[0:4, :]
    for grp, k, d in near:
        if d < 2:
            pltpu.make_async_remote_copy(
                rest.at[pl.ds(0, 4)], gather_rest.at[d * domains + j, pl.ds(0, 4)], send_sem.at[3], recv_sem.at[5 + d],
                device_id=(grp, domain(k)), device_id_type=MESH,
            ).start()
    halo_bc[...] = jnp.broadcast_to(halo_row, (blocks, blocks)).T
    for c in range(3):
        shift_bc[c] = jnp.broadcast_to(s[c], (blocks, blocks)).T

    def arrived(d):
        n = domains - 1 if d == 1 else domains
        span = gather.at[pl.ds(d * domains, n), pl.ds(0, 9)]
        pltpu.make_async_copy(span, span, recv_sem.at[d]).wait()

    def rest_arrived(d):
        n = domains - 1 if d == 1 else domains
        span = gather_rest.at[pl.ds(d * domains, n), pl.ds(0, 4)]
        pltpu.make_async_copy(span, span, recv_sem.at[5 + d]).wait()

    def hot(values, row):
        return jnp.concatenate(
            [jnp.where(values == r, 1.0, 0.0).astype(jnp.bfloat16) for r in row], axis=1
        )

    def parts(values):
        return jnp.concatenate([in_three(v).astype(jnp.bfloat16) for v in values], axis=1)

    def slot_of(d):
        return [d * domains + k for k in range(domains)]

    def summed(d):
        return lax.dot_general(
            hot(halo_bc[...], [gather[q, 8:9, :] for q in slot_of(d)]),
            parts([gather[q, 0:8, :] for q in slot_of(d)]),
            NT, preferred_element_type=F32,
        )

    def owned(d):
        mine = (iota((blocks, blocks), 0) + me * blocks).astype(F32)
        values = [
            jnp.concatenate([gather[q, 0:8, :], gather_rest[q, 0:8, :]], axis=0) for q in slot_of(d)
        ]
        return lax.dot_general(
            parts(values), hot(mine, [gather_rest[q, 0:1, :] for q in slot_of(d)]),
            NT, preferred_element_type=F32,
        )

    arrived(2)
    stats = summed(2)
    arrived(0)
    stats = stats + summed(0)
    arrived(1)
    stats = stats + summed(1)
    stats = stats[:, 0:8] + stats[:, 8:16] + stats[:, 16:24]
    wide = [jnp.broadcast_to(stats[:, k : k + 1], (blocks, 128)) for k in range(8)]
    heavy = 1.0 / jnp.maximum(wide[0], 1.0)
    drift = [wide[4 + c] * heavy for c in range(3)]
    spread = wide[7] * heavy - (drift[0] * drift[0] + drift[1] * drift[1] + drift[2] * drift[2])
    over = 1.0 / (3.0 * spread + EPSILON)
    centre = [wide[1 + c] * heavy - shift_bc[c] for c in range(3)]

    for i in range(blocks // 8):
        r = slice(8 * i, 8 * i + 8)
        alive = live_bc[r, :]
        for t in range(tiles):
            q = slice(128 * t, 128 * t + 128)
            mask = (lane + t * 128).astype(F32) < alive
            dv = [vel[c, r, q] - drift[c][r] for c in range(3)]
            dp = [pos[c, r, q] - centre[c][r] for c in range(3)]
            kin = (dv[0] * dv[0] + dv[1] * dv[1] + dv[2] * dv[2]) * over[r]
            rad = dp[0] * dp[0] + dp[1] * dp[1] + dp[2] * dp[2]
            kin_ref[r, q] = jnp.where(mask, kin, 0.0)
            rad_ref[r, q] = jnp.where(mask, rad, 0.0)

    rest_arrived(1)
    rest_arrived(0)
    table_sums = owned(1) + owned(0)
    own = table_sums[0:16] + table_sums[16:32] + table_sums[32:48]
    heavy = jnp.maximum(own[0:1], 1.0)
    c = [own[1 + i : 2 + i] / heavy for i in range(3)]
    d = [own[4 + i : 5 + i] / heavy for i in range(3)]
    spread = own[7:8] / heavy - (d[0] * d[0] + d[1] * d[1] + d[2] * d[2])
    spin = [
        own[9:10] / heavy - (c[1] * d[2] - c[2] * d[1]),
        own[10:11] / heavy - (c[2] * d[0] - c[0] * d[2]),
        own[11:12] / heavy - (c[0] * d[1] - c[1] * d[0]),
    ]

    def served(r):
        share = min(2, roots)
        return [p for p in range(roots, depth) if roots - 1 - (p - roots) * share // (depth - roots) == r]

    def tell(there, a, k):
        return pltpu.make_async_remote_copy(
            line, line, send_sem.at[2], recv_sem.at[4],
            device_id=(there * planes_groups + a, k), device_id_type=MESH,
        )

    @pl.when(is_root)
    def _():
        others = masses.at[pl.ds(0, everyone - 1)]
        pltpu.make_async_copy(others, others, recv_sem.at[3]).wait()
        rows = masses[...].reshape(everyone // 8, 8, blocks)
        line[...] = jnp.sum(jnp.sum(rows, axis=0), axis=0, keepdims=True)
        for a in range(planes_groups):
            for k in range(domains):
                if (a, k) != (0, ROOT):
                    tell(z, a, k).start()
        for r in range(roots):
            @pl.when(z == r)
            def _():
                for there in served(r):
                    for a in range(planes_groups):
                        for k in range(domains):
                            tell(there, a, k).start()

    @pl.when(jnp.logical_not(is_root))
    def _():
        pltpu.make_async_copy(line, line, recv_sem.at[4]).wait()

    total = jnp.sum(line[...], axis=1, keepdims=True)
    share = own[0:1] * float(groups * domains * blocks) / total
    table_ref[...] = jnp.concatenate([share, *c, *d, spread, *spin], axis=0)

    @pl.when(is_root)
    def _():
        for r in range(roots):
            @pl.when(z == r)
            def _():
                told = masses.at[pl.ds(0, (1 + len(served(r))) * planes_groups * domains - 1)]
                pltpu.make_async_copy(told, told, send_sem.at[2]).wait()

        sent = masses.at[pl.ds(0, roots - 1)]
        pltpu.make_async_copy(sent, sent, send_sem.at[0]).wait()

    @pl.when(jnp.logical_not(is_root))
    def _():
        sent = masses.at[pl.ds(0, roots)]
        pltpu.make_async_copy(sent, sent, send_sem.at[0]).wait()

    n_near = len(near)
    sent = gather.at[pl.ds(0, n_near), pl.ds(0, 9)]
    pltpu.make_async_copy(sent, sent, send_sem.at[1]).wait()
    sent = gather_rest.at[pl.ds(0, 2 * domains - 1), pl.ds(0, 4)]
    pltpu.make_async_copy(sent, sent, send_sem.at[3]).wait()


def flush(table_ref, kin_ref, rad_ref, table_hbm, kin_hbm, rad_hbm, sem):
    pairs = ((kin_ref, kin_hbm), (rad_ref, rad_hbm), (table_ref, table_hbm))
    copies = [pltpu.make_async_copy(a, b, sem.at[i]) for i, (a, b) in enumerate(pairs)]
    for copy in copies:
        copy.start()
    for copy in copies:
        copy.wait()


def solution(mesh, plane_groups=PLANE_GROUPS):
    groups, domains = mesh.shape["grp"], mesh.shape["dom"]
    both = ("grp", "dom")

    def local(positions, velocities, masses, block_halo, block_shift, block_live, block_count, home_slot):
        blocks, width = masses.shape
        hbm = pl.BlockSpec(memory_space=pltpu.HBM)
        vmem = pl.BlockSpec(memory_space=pltpu.VMEM)
        long = home_slot.shape[0] // 128
        results = pl.pallas_call(
            functools.partial(kernel, (groups, domains, plane_groups)),
            out_shape=(
                pltpu.VMEM((11, blocks), F32),
                pltpu.VMEM((blocks, width), F32),
                pltpu.VMEM((blocks, width), F32),
            ),
            in_specs=[hbm] * 8,
            out_specs=(vmem, vmem, vmem),
            scratch_shapes=[
                pltpu.VMEM((3, blocks, width), F32),
                pltpu.VMEM((3, blocks, width), F32),
                pltpu.VMEM((blocks, width), F32),
                pltpu.VMEM((1, blocks), jnp.int32),
                pltpu.VMEM((3, blocks), jnp.int32),
                pltpu.VMEM((1, blocks), jnp.int32),
                pltpu.VMEM((1, 1), jnp.int32),
                pltpu.VMEM((long, 128), jnp.int32),
                pltpu.VMEM((blocks, blocks), F32),
                pltpu.VMEM((blocks, blocks), F32),
                pltpu.VMEM((3, blocks, blocks), F32),
                pltpu.VMEM((16, blocks), F32),
                pltpu.VMEM((8, blocks), F32),
                pltpu.VMEM((3 * domains, 16, blocks), F32),
                pltpu.VMEM((2 * domains, 8, blocks), F32),
                pltpu.VMEM((groups * domains, blocks), F32),
                pltpu.VMEM((1, blocks), F32),
                pltpu.SemaphoreType.DMA((3 * CHUNKS,)),
                pltpu.SemaphoreType.DMA((4,)),
                pltpu.SemaphoreType.DMA,
                pltpu.SemaphoreType.DMA((4,)),
                pltpu.SemaphoreType.DMA((7,)),
            ],
            compiler_params=pltpu.CompilerParams(collective_id=0, has_side_effects=True),
        )(
            positions, velocities, masses,
            block_halo.reshape(1, blocks), block_shift, block_live.reshape(1, blocks), block_count.reshape(1, 1),
            home_slot.reshape(long, 128),
        )
        return pl.pallas_call(
            flush,
            out_shape=tuple(jax.ShapeDtypeStruct(r.shape, F32) for r in results),
            in_specs=[vmem] * 3,
            out_specs=(hbm,) * 3,
            scratch_shapes=[pltpu.SemaphoreType.DMA((3,))],
        )(*[pltpu.with_memory_space_constraint(r, pltpu.VMEM) for r in results])

    return jax.shard_map(
        local,
        mesh=mesh,
        in_specs=(
            P(None, both, None), P(None, both, None), P(both, None), P(both), P(None, both), P(both), P(both), P(),
        ),
        out_specs=(P(None, both), P(both, None), P(both, None)),
        check_vma=False,
    )
```

```python
import functools

import jax
import jax.numpy as jnp
from jax import lax
from jax.experimental import pallas as pl
from jax.experimental.pallas import tpu as pltpu
from jax.sharding import PartitionSpec as P

MESH = pl.DeviceIdType.MESH
EPSILON = 1e-6
PLANE_GROUPS = 4
ROOT = 1
CHUNKS = 4
F32 = jnp.float32
NT = (((1,), (1,)), ((), ()))


def wrapped(index, size):
    return jnp.where(index >= size, index - size, index)


def iota(shape, dim):
    return lax.broadcasted_iota(jnp.int32, shape, dim)


def in_three(x):
    high = x.astype(jnp.bfloat16).astype(F32)
    rest = x - high
    middle = rest.astype(jnp.bfloat16).astype(F32)
    return jnp.concatenate([high, middle, rest - middle], axis=0)


def roots_of(depth, planes_groups, domains):
    half = depth // 2
    second = (ROOT + 2) % domains if domains > 2 else 0
    plane = [(a, k) for a in range(planes_groups) for k in range(domains)]
    tree = [((0, 0, ROOT), []), ((0, 0, second), [(0, 0, k) for k in range(domains) if k not in (ROOT, second)])]
    tree += [((0, a, ROOT), [(0, a, k) for k in range(domains) if k != ROOT]) for a in range(1, planes_groups)]
    share = max(1, min(2, half - 1))
    for r in range(1, half):
        late = [p for p in range(half, depth) if half - 1 - (p - half) * share // (depth - half) == r]
        tree.append(((r, 0, ROOT), [(p, a, k) for p in [r] + late for a, k in plane if (p, a, k) != (r, 0, ROOT)]))
    return tree


def kernel(
    sizes,
    pos_hbm, vel_hbm, mass_hbm, halo_hbm, shift_hbm, live_hbm, count_hbm, slot_hbm,
    table_ref, kin_ref, rad_ref,
    pos, vel, mass, halo, shift, live, count, slots,
    live_bc, halo_bc, shift_bc, moments, rest, gather, gather_rest, masses, line,
    in_sem, small_sem, count_sem, send_sem, recv_sem,
):
    groups, domains, planes_groups = sizes
    blocks = mass.shape[0]
    width = mass.shape[1]
    depth = groups // planes_groups
    g, j = lax.axis_index("grp"), lax.axis_index("dom")
    z = g // planes_groups
    x = g - z * planes_groups
    nxt = wrapped(g + 1, groups)
    prv = jnp.where(g == 0, groups - 1, g - 1)

    order = sorted(range(domains), key=lambda k: -min(k, domains - k))
    near = [(nxt, k, 0) for k in order] + [(prv, k, 2) for k in order] + [(g, k, 1) for k in order if k]
    me = g * domains + j
    everyone = groups * domains
    tree = roots_of(depth, planes_groups, domains)
    n_roots = len(tree)
    i_am = [(g == there * planes_groups + a) & (j == k) for (there, a, k), _ in tree]
    is_root = functools.reduce(jnp.logical_or, i_am)

    def domain(k):
        return wrapped(j + k, domains)

    def greet(grp, dom):
        pl.semaphore_signal(barrier, inc=1, device_id=(grp, dom), device_id_type=MESH)

    small = [
        pltpu.make_async_copy(live_hbm, live, small_sem.at[0]),
        pltpu.make_async_copy(count_hbm, count, count_sem),
        pltpu.make_async_copy(halo_hbm, halo, small_sem.at[1]),
        pltpu.make_async_copy(shift_hbm, shift, small_sem.at[2]),
        pltpu.make_async_copy(slot_hbm, slots, small_sem.at[3]),
    ]
    for copy in small[:2]:
        copy.start()
    part = blocks // CHUNKS
    big = []
    for c in range(CHUNKS):
        rows = pl.ds(c * part, part)
        big.append([
            pltpu.make_async_copy(mass_hbm.at[rows], mass.at[rows], in_sem.at[3 * c]),
            pltpu.make_async_copy(pos_hbm.at[:, rows], pos.at[:, rows], in_sem.at[3 * c + 1]),
            pltpu.make_async_copy(vel_hbm.at[:, rows], vel.at[:, rows], in_sem.at[3 * c + 2]),
        ])
        for copy in big[-1]:
            copy.start()

    for copy in small[2:]:
        copy.start()
    barrier = pltpu.get_barrier_semaphore()
    for grp, k, _ in near:
        greet(grp, domain(k))

    @pl.when(is_root)
    def _():
        @pl.loop(0, depth)
        def _(step):
            there = depth - 1 - step
            for a in range(planes_groups):
                for k in range(domains):
                    if (a, k) in {root[1:] for root, _ in tree}:
                        @pl.when((there * planes_groups + a != g) | (j != k))
                        def _():
                            greet(there * planes_groups + a, k)
                    else:
                        greet(there * planes_groups + a, k)

    for copy in small[:2]:
        copy.wait()

    row = iota((1, blocks), 1)
    live_row = jnp.where(row < count[...], live[...], 0).astype(F32)
    live_bc[...] = jnp.broadcast_to(live_row, (blocks, blocks)).T

    tiles = width // 128
    lane = iota((8, 128), 1)
    diagonal = lane - iota((8, 128), 0)

    def moment_step(i, sums):
        base = pl.multiple_of(i * 8, 8)
        rows = pl.ds(base, 8)
        alive = live_bc[rows, :]
        acc = None
        for t in range(tiles):
            cols = pl.ds(t * 128, 128)
            w = jnp.where((lane + t * 128).astype(F32) < alive, mass[rows, cols], 0.0)
            p = [pos[c, rows, cols] for c in range(3)]
            v = [vel[c, rows, cols] for c in range(3)]
            wv = [w * v[c] for c in range(3)]
            terms = [w] + [w * p[c] for c in range(3)] + wv
            terms.append(wv[0] * v[0] + wv[1] * v[1] + wv[2] * v[2])
            terms.append(p[1] * wv[2] - p[2] * wv[1])
            terms.append(p[2] * wv[0] - p[0] * wv[2])
            terms.append(p[0] * wv[1] - p[1] * wv[0])
            acc = terms if acc is None else [a + b for a, b in zip(acc, terms)]
        here = diagonal == base
        return tuple(
            s + jnp.where(here, jnp.sum(a, axis=1, keepdims=True), 0.0)
            for s, a in zip(sums, acc)
        )

    sums = tuple(jnp.zeros((8, 128), F32) for _ in range(11))
    for c in range(CHUNKS):
        for copy in big[c]:
            copy.wait()
        sums = lax.fori_loop(c * part // 8, (c + 1) * part // 8, moment_step, sums, unroll=4)
    for copy in small[2:]:
        copy.wait()
    halo_row = halo[...].astype(F32)
    shift_rows = shift[...].astype(F32)
    m = [jnp.sum(s, axis=0, keepdims=True) for s in sums]
    s = [shift_rows[c : c + 1] for c in range(3)]
    raw_p, mom_v = m[1:4], m[4:7]
    ang = [
        m[8] + (s[1] * mom_v[2] - s[2] * mom_v[1]),
        m[9] + (s[2] * mom_v[0] - s[0] * mom_v[2]),
        m[10] + (s[0] * mom_v[1] - s[1] * mom_v[0]),
    ]
    place = [raw_p[c] + s[c] * m[0] for c in range(3)]

    moments[0:9, :] = jnp.concatenate([m[0], *place, *mom_v, m[7], halo_row], axis=0)
    gather[domains + j, 0:9, :] = moments[0:9, :]
    masses[pl.ds(me, 1), :] = m[0]

    pl.semaphore_wait(barrier, jnp.where(is_root, len(near) + n_roots - 1, len(near) + n_roots))

    for mine, ((there, a, k), _) in zip(i_am, tree):
        @pl.when(jnp.logical_not(mine))
        def _():
            pltpu.make_async_remote_copy(
                moments.at[pl.ds(0, 1)], masses.at[pl.ds(me, 1)], send_sem.at[0], recv_sem.at[3],
                device_id=(there * planes_groups + a, k), device_id_type=MESH,
            ).start()

    for grp, k, d in near:
        pltpu.make_async_remote_copy(
            moments.at[pl.ds(0, 9)], gather.at[d * domains + j, pl.ds(0, 9)], send_sem.at[1], recv_sem.at[d],
            device_id=(grp, domain(k)), device_id_type=MESH,
        ).start()
    halo_int = halo[...]
    high_bits = halo_int // 128
    low_bits = halo_int - high_bits * 128
    table = slots[...]
    table_high = table // 256
    table_low = table - table_high * 256
    pick = jnp.where(iota((128, blocks), 0) == low_bits, 1.0, 0.0).astype(jnp.bfloat16)
    picked = jnp.dot(
        jnp.concatenate([table_high, table_low], axis=0).astype(F32).astype(jnp.bfloat16),
        pick,
        preferred_element_type=F32,
    )
    long = table.shape[0]
    both = picked[:long] * 256.0 + picked[long:]
    slot_row = jnp.sum(
        jnp.where(iota((long, blocks), 0) == high_bits, both, 0.0), axis=0, keepdims=True
    )

    rest[0:4, :] = jnp.concatenate([slot_row, *ang], axis=0)
    gather_rest[domains + j, 0:4, :] = rest[0:4, :]
    for grp, k, d in near:
        if d < 2:
            pltpu.make_async_remote_copy(
                rest.at[pl.ds(0, 4)], gather_rest.at[d * domains + j, pl.ds(0, 4)], send_sem.at[3], recv_sem.at[5 + d],
                device_id=(grp, domain(k)), device_id_type=MESH,
            ).start()
    halo_bc[...] = jnp.broadcast_to(halo_row, (blocks, blocks)).T
    for c in range(3):
        shift_bc[c] = jnp.broadcast_to(s[c], (blocks, blocks)).T

    def arrived(d):
        n = domains - 1 if d == 1 else domains
        span = gather.at[pl.ds(d * domains, n), pl.ds(0, 9)]
        pltpu.make_async_copy(span, span, recv_sem.at[d]).wait()

    def rest_arrived(d):
        n = domains - 1 if d == 1 else domains
        span = gather_rest.at[pl.ds(d * domains, n), pl.ds(0, 4)]
        pltpu.make_async_copy(span, span, recv_sem.at[5 + d]).wait()

    def hot(values, row):
        return jnp.concatenate(
            [jnp.where(values == r, 1.0, 0.0).astype(jnp.bfloat16) for r in row], axis=1
        )

    def parts(values):
        return jnp.concatenate([in_three(v).astype(jnp.bfloat16) for v in values], axis=1)

    def slot_of(d):
        return [d * domains + k for k in range(domains)]

    def summed(d):
        return lax.dot_general(
            hot(halo_bc[...], [gather[q, 8:9, :] for q in slot_of(d)]),
            parts([gather[q, 0:8, :] for q in slot_of(d)]),
            NT, preferred_element_type=F32,
        )

    def owned(d):
        mine = (iota((blocks, blocks), 0) + me * blocks).astype(F32)
        values = [
            jnp.concatenate([gather[q, 0:8, :], gather_rest[q, 0:8, :]], axis=0) for q in slot_of(d)
        ]
        return lax.dot_general(
            parts(values), hot(mine, [gather_rest[q, 0:1, :] for q in slot_of(d)]),
            NT, preferred_element_type=F32,
        )

    arrived(2)
    stats = summed(2)
    arrived(0)
    stats = stats + summed(0)
    rest_arrived(0)
    table_sums = owned(0)
    arrived(1)
    stats = stats + summed(1)
    stats = stats[:, 0:8] + stats[:, 8:16] + stats[:, 16:24]
    wide = [jnp.broadcast_to(stats[:, k : k + 1], (blocks, 128)) for k in range(8)]
    heavy = 1.0 / jnp.maximum(wide[0], 1.0)
    drift = [wide[4 + c] * heavy for c in range(3)]
    spread = wide[7] * heavy - (drift[0] * drift[0] + drift[1] * drift[1] + drift[2] * drift[2])
    over = 1.0 / (3.0 * spread + EPSILON)
    centre = [wide[1 + c] * heavy - shift_bc[c] for c in range(3)]

    for i in range(blocks // 8):
        r = slice(8 * i, 8 * i + 8)
        alive = live_bc[r, :]
        for t in range(tiles):
            q = slice(128 * t, 128 * t + 128)
            mask = (lane + t * 128).astype(F32) < alive
            dv = [vel[c, r, q] - drift[c][r] for c in range(3)]
            dp = [pos[c, r, q] - centre[c][r] for c in range(3)]
            kin = (dv[0] * dv[0] + dv[1] * dv[1] + dv[2] * dv[2]) * over[r]
            rad = dp[0] * dp[0] + dp[1] * dp[1] + dp[2] * dp[2]
            kin_ref[r, q] = jnp.where(mask, kin, 0.0)
            rad_ref[r, q] = jnp.where(mask, rad, 0.0)

    rest_arrived(1)
    table_sums = table_sums + owned(1)
    own = table_sums[0:16] + table_sums[16:32] + table_sums[32:48]
    heavy = jnp.maximum(own[0:1], 1.0)
    c = [own[1 + i : 2 + i] / heavy for i in range(3)]
    d = [own[4 + i : 5 + i] / heavy for i in range(3)]
    spread = own[7:8] / heavy - (d[0] * d[0] + d[1] * d[1] + d[2] * d[2])
    spin = [
        own[9:10] / heavy - (c[1] * d[2] - c[2] * d[1]),
        own[10:11] / heavy - (c[2] * d[0] - c[0] * d[2]),
        own[11:12] / heavy - (c[0] * d[1] - c[1] * d[0]),
    ]

    def tell(there, a, k):
        return pltpu.make_async_remote_copy(
            line, line, send_sem.at[2], recv_sem.at[4],
            device_id=(there * planes_groups + a, k), device_id_type=MESH,
        )

    @pl.when(is_root)
    def _():
        others = masses.at[pl.ds(0, everyone - 1)]
        pltpu.make_async_copy(others, others, recv_sem.at[3]).wait()
        rows = masses[...].reshape(everyone // 8, 8, blocks)
        line[...] = jnp.sum(jnp.sum(rows, axis=0), axis=0, keepdims=True)

    for mine, (_, clients) in zip(i_am, tree):
        if clients:
            @pl.when(mine)
            def _():
                for client in clients:
                    tell(*client).start()

    @pl.when(jnp.logical_not(is_root))
    def _():
        pltpu.make_async_copy(line, line, recv_sem.at[4]).wait()

    total = jnp.sum(line[...], axis=1, keepdims=True)
    share = own[0:1] * float(groups * domains * blocks) / total
    table_ref[...] = jnp.concatenate([share, *c, *d, spread, *spin], axis=0)

    @pl.when(is_root)
    def _():
        sent = masses.at[pl.ds(0, n_roots - 1)]
        pltpu.make_async_copy(sent, sent, send_sem.at[0]).wait()

    for mine, (_, clients) in zip(i_am, tree):
        if clients:
            @pl.when(mine)
            def _():
                told = masses.at[pl.ds(0, len(clients))]
                pltpu.make_async_copy(told, told, send_sem.at[2]).wait()

    @pl.when(jnp.logical_not(is_root))
    def _():
        sent = masses.at[pl.ds(0, n_roots)]
        pltpu.make_async_copy(sent, sent, send_sem.at[0]).wait()

    n_near = len(near)
    sent = gather.at[pl.ds(0, n_near), pl.ds(0, 9)]
    pltpu.make_async_copy(sent, sent, send_sem.at[1]).wait()
    sent = gather_rest.at[pl.ds(0, 2 * domains - 1), pl.ds(0, 4)]
    pltpu.make_async_copy(sent, sent, send_sem.at[3]).wait()


def flush(table_ref, kin_ref, rad_ref, table_hbm, kin_hbm, rad_hbm, sem):
    pairs = ((kin_ref, kin_hbm), (rad_ref, rad_hbm), (table_ref, table_hbm))
    copies = [pltpu.make_async_copy(a, b, sem.at[i]) for i, (a, b) in enumerate(pairs)]
    for copy in copies:
        copy.start()
    for copy in copies:
        copy.wait()


def solution(mesh, plane_groups=PLANE_GROUPS):
    groups, domains = mesh.shape["grp"], mesh.shape["dom"]
    both = ("grp", "dom")

    def local(positions, velocities, masses, block_halo, block_shift, block_live, block_count, home_slot):
        blocks, width = masses.shape
        hbm = pl.BlockSpec(memory_space=pltpu.HBM)
        vmem = pl.BlockSpec(memory_space=pltpu.VMEM)
        long = home_slot.shape[0] // 128
        results = pl.pallas_call(
            functools.partial(kernel, (groups, domains, plane_groups)),
            out_shape=(
                pltpu.VMEM((11, blocks), F32),
                pltpu.VMEM((blocks, width), F32),
                pltpu.VMEM((blocks, width), F32),
            ),
            in_specs=[hbm] * 8,
            out_specs=(vmem, vmem, vmem),
            scratch_shapes=[
                pltpu.VMEM((3, blocks, width), F32),
                pltpu.VMEM((3, blocks, width), F32),
                pltpu.VMEM((blocks, width), F32),
                pltpu.VMEM((1, blocks), jnp.int32),
                pltpu.VMEM((3, blocks), jnp.int32),
                pltpu.VMEM((1, blocks), jnp.int32),
                pltpu.VMEM((1, 1), jnp.int32),
                pltpu.VMEM((long, 128), jnp.int32),
                pltpu.VMEM((blocks, blocks), F32),
                pltpu.VMEM((blocks, blocks), F32),
                pltpu.VMEM((3, blocks, blocks), F32),
                pltpu.VMEM((16, blocks), F32),
                pltpu.VMEM((8, blocks), F32),
                pltpu.VMEM((3 * domains, 16, blocks), F32),
                pltpu.VMEM((2 * domains, 8, blocks), F32),
                pltpu.VMEM((groups * domains, blocks), F32),
                pltpu.VMEM((1, blocks), F32),
                pltpu.SemaphoreType.DMA((3 * CHUNKS,)),
                pltpu.SemaphoreType.DMA((4,)),
                pltpu.SemaphoreType.DMA,
                pltpu.SemaphoreType.DMA((4,)),
                pltpu.SemaphoreType.DMA((7,)),
            ],
            compiler_params=pltpu.CompilerParams(collective_id=0, has_side_effects=True),
        )(
            positions, velocities, masses,
            block_halo.reshape(1, blocks), block_shift, block_live.reshape(1, blocks), block_count.reshape(1, 1),
            home_slot.reshape(long, 128),
        )
        return pl.pallas_call(
            flush,
            out_shape=tuple(jax.ShapeDtypeStruct(r.shape, F32) for r in results),
            in_specs=[vmem] * 3,
            out_specs=(hbm,) * 3,
            scratch_shapes=[pltpu.SemaphoreType.DMA((3,))],
        )(*[pltpu.with_memory_space_constraint(r, pltpu.VMEM) for r in results])

    return jax.shard_map(
        local,
        mesh=mesh,
        in_specs=(
            P(None, both, None), P(None, both, None), P(both, None), P(both), P(None, both), P(both), P(both), P(),
        ),
        out_specs=(P(None, both), P(both, None), P(both, None)),
        check_vma=False,
    )
```

```python
import functools

import jax
import jax.numpy as jnp
from jax import lax
from jax.experimental import pallas as pl
from jax.experimental.pallas import tpu as pltpu
from jax.sharding import PartitionSpec as P

MESH = pl.DeviceIdType.MESH
EPSILON = 1e-6
PLANE_GROUPS = 4
ROOT = 1
CHUNKS = 4
F32 = jnp.float32
NT = (((1,), (1,)), ((), ()))


def wrapped(index, size):
    return jnp.where(index >= size, index - size, index)


def iota(shape, dim):
    return lax.broadcasted_iota(jnp.int32, shape, dim)


def in_three(x):
    high = x.astype(jnp.bfloat16).astype(F32)
    rest = x - high
    middle = rest.astype(jnp.bfloat16).astype(F32)
    return jnp.concatenate([high, middle, rest - middle], axis=0)


def roots_of(depth, planes_groups, domains):
    half = max(2, depth * 3 // 8)
    plane = [(a, k) for a in range(planes_groups) for k in range(domains)]
    tree = [((0, 0, 0), []), ((0, 0, ROOT), [])]
    if domains > 2:
        tree.append(((0, 0, 3), [(0, 0, k) for k in range(2, domains - 2) if k != 3]))
        tree.append(((0, 0, domains - 1), [(0, 0, domains - 2)]))
    tree += [((0, a, ROOT), [(0, a, k) for k in range(domains) if k != ROOT]) for a in range(1, planes_groups)]
    share = max(1, min(2, half - 1))
    for r in range(1, half):
        late = [p for p in range(half, depth) if half - 1 - (p - half) * share // (depth - half) == r]
        tree.append(((r, 0, ROOT), [(p, a, k) for p in [r] + late for a, k in plane if (p, a, k) != (r, 0, ROOT)]))
    return tree


def kernel(
    sizes,
    pos_hbm, vel_hbm, mass_hbm, halo_hbm, shift_hbm, live_hbm, count_hbm, slot_hbm,
    table_ref, kin_ref, rad_ref,
    pos, vel, mass, halo, shift, live, count, slots,
    live_bc, halo_bc, shift_bc, moments, rest, gather, gather_rest, mine_all, masses, line,
    in_sem, small_sem, count_sem, send_sem, recv_sem,
):
    groups, domains, planes_groups = sizes
    blocks = mass.shape[0]
    width = mass.shape[1]
    depth = groups // planes_groups
    g, j = lax.axis_index("grp"), lax.axis_index("dom")
    z = g // planes_groups
    x = g - z * planes_groups
    nxt = wrapped(g + 1, groups)
    prv = jnp.where(g == 0, groups - 1, g - 1)

    order = sorted(range(domains), key=lambda k: -min(k, domains - k))
    near = [(nxt, k, 0) for k in order] + [(prv, k, 2) for k in order] + [(g, k, 1) for k in order if k]
    me = g * domains + j
    everyone = groups * domains
    tree = roots_of(depth, planes_groups, domains)
    n_roots = len(tree)
    i_am = [(g == there * planes_groups + a) & (j == k) for (there, a, k), _ in tree]
    is_root = functools.reduce(jnp.logical_or, i_am)

    def domain(k):
        return wrapped(j + k, domains)

    def greet(grp, dom):
        pl.semaphore_signal(barrier, inc=1, device_id=(grp, dom), device_id_type=MESH)

    small = [
        pltpu.make_async_copy(live_hbm, live, small_sem.at[0]),
        pltpu.make_async_copy(count_hbm, count, count_sem),
        pltpu.make_async_copy(halo_hbm, halo, small_sem.at[1]),
        pltpu.make_async_copy(shift_hbm, shift, small_sem.at[2]),
        pltpu.make_async_copy(slot_hbm, slots, small_sem.at[3]),
    ]
    for copy in small[:2]:
        copy.start()
    part = blocks // CHUNKS
    big = []
    for c in range(CHUNKS):
        rows = pl.ds(c * part, part)
        big.append([
            pltpu.make_async_copy(mass_hbm.at[rows], mass.at[rows], in_sem.at[3 * c]),
            pltpu.make_async_copy(pos_hbm.at[:, rows], pos.at[:, rows], in_sem.at[3 * c + 1]),
            pltpu.make_async_copy(vel_hbm.at[:, rows], vel.at[:, rows], in_sem.at[3 * c + 2]),
        ])
        for copy in big[-1]:
            copy.start()

    for copy in small[2:]:
        copy.start()
    barrier = pltpu.get_barrier_semaphore()
    for grp, k, _ in near:
        greet(grp, domain(k))

    @pl.when(is_root)
    def _():
        @pl.loop(0, depth)
        def _(step):
            there = depth - 1 - step
            for a in range(planes_groups):
                for k in range(domains):
                    if (a, k) in {root[1:] for root, _ in tree}:
                        @pl.when((there * planes_groups + a != g) | (j != k))
                        def _():
                            greet(there * planes_groups + a, k)
                    else:
                        greet(there * planes_groups + a, k)

    for copy in small[:2]:
        copy.wait()

    row = iota((1, blocks), 1)
    live_row = jnp.where(row < count[...], live[...], 0).astype(F32)
    live_bc[...] = jnp.broadcast_to(live_row, (blocks, blocks)).T

    tiles = width // 128
    lane = iota((8, 128), 1)
    diagonal = lane - iota((8, 128), 0)

    def moment_step(i, sums):
        base = pl.multiple_of(i * 8, 8)
        rows = pl.ds(base, 8)
        alive = live_bc[rows, :]
        acc = None
        for t in range(tiles):
            cols = pl.ds(t * 128, 128)
            w = jnp.where((lane + t * 128).astype(F32) < alive, mass[rows, cols], 0.0)
            p = [pos[c, rows, cols] for c in range(3)]
            v = [vel[c, rows, cols] for c in range(3)]
            wv = [w * v[c] for c in range(3)]
            terms = [w] + [w * p[c] for c in range(3)] + wv
            terms.append(wv[0] * v[0] + wv[1] * v[1] + wv[2] * v[2])
            terms.append(p[1] * wv[2] - p[2] * wv[1])
            terms.append(p[2] * wv[0] - p[0] * wv[2])
            terms.append(p[0] * wv[1] - p[1] * wv[0])
            acc = terms if acc is None else [a + b for a, b in zip(acc, terms)]
        here = diagonal == base
        return tuple(
            s + jnp.where(here, jnp.sum(a, axis=1, keepdims=True), 0.0)
            for s, a in zip(sums, acc)
        )

    sums = tuple(jnp.zeros((8, 128), F32) for _ in range(11))
    for c in range(CHUNKS):
        for copy in big[c]:
            copy.wait()
        sums = lax.fori_loop(c * part // 8, (c + 1) * part // 8, moment_step, sums, unroll=4)
    for copy in small[2:]:
        copy.wait()
    halo_row = halo[...].astype(F32)
    shift_rows = shift[...].astype(F32)
    m = [jnp.sum(s, axis=0, keepdims=True) for s in sums]
    s = [shift_rows[c : c + 1] for c in range(3)]
    raw_p, mom_v = m[1:4], m[4:7]
    ang = [
        m[8] + (s[1] * mom_v[2] - s[2] * mom_v[1]),
        m[9] + (s[2] * mom_v[0] - s[0] * mom_v[2]),
        m[10] + (s[0] * mom_v[1] - s[1] * mom_v[0]),
    ]
    place = [raw_p[c] + s[c] * m[0] for c in range(3)]

    moments[0:9, :] = jnp.concatenate([m[0], *place, *mom_v, m[7], halo_row], axis=0)
    gather[domains + j, 0:9, :] = moments[0:9, :]
    whole = jnp.broadcast_to(jnp.sum(m[0], axis=1, keepdims=True), (1, blocks))
    mine_all[...] = whole
    masses[pl.ds(me, 1), :] = whole

    pl.semaphore_wait(barrier, jnp.where(is_root, len(near) + n_roots - 1, len(near) + n_roots))

    for mine, ((there, a, k), _) in zip(i_am, tree):
        @pl.when(jnp.logical_not(mine))
        def _():
            pltpu.make_async_remote_copy(
                mine_all, masses.at[pl.ds(me, 1)], send_sem.at[0], recv_sem.at[3],
                device_id=(there * planes_groups + a, k), device_id_type=MESH,
            ).start()

    for grp, k, d in near:
        pltpu.make_async_remote_copy(
            moments.at[pl.ds(0, 9)], gather.at[d * domains + j, pl.ds(0, 9)], send_sem.at[1], recv_sem.at[d],
            device_id=(grp, domain(k)), device_id_type=MESH,
        ).start()
    halo_int = halo[...]
    high_bits = halo_int // 128
    low_bits = halo_int - high_bits * 128
    table = slots[...]
    table_high = table // 256
    table_low = table - table_high * 256
    pick = jnp.where(iota((128, blocks), 0) == low_bits, 1.0, 0.0).astype(jnp.bfloat16)
    picked = jnp.dot(
        jnp.concatenate([table_high, table_low], axis=0).astype(F32).astype(jnp.bfloat16),
        pick,
        preferred_element_type=F32,
    )
    long = table.shape[0]
    both = picked[:long] * 256.0 + picked[long:]
    slot_row = jnp.sum(
        jnp.where(iota((long, blocks), 0) == high_bits, both, 0.0), axis=0, keepdims=True
    )

    rest[0:4, :] = jnp.concatenate([slot_row, *ang], axis=0)
    gather_rest[domains + j, 0:4, :] = rest[0:4, :]
    for grp, k, d in near:
        if d < 2:
            pltpu.make_async_remote_copy(
                rest.at[pl.ds(0, 4)], gather_rest.at[d * domains + j, pl.ds(0, 4)], send_sem.at[3], recv_sem.at[5 + d],
                device_id=(grp, domain(k)), device_id_type=MESH,
            ).start()
    halo_bc[...] = jnp.broadcast_to(halo_row, (blocks, blocks)).T
    for c in range(3):
        shift_bc[c] = jnp.broadcast_to(s[c], (blocks, blocks)).T

    def arrived(d):
        n = domains - 1 if d == 1 else domains
        span = gather.at[pl.ds(d * domains, n), pl.ds(0, 9)]
        pltpu.make_async_copy(span, span, recv_sem.at[d]).wait()

    def rest_arrived(d):
        n = domains - 1 if d == 1 else domains
        span = gather_rest.at[pl.ds(d * domains, n), pl.ds(0, 4)]
        pltpu.make_async_copy(span, span, recv_sem.at[5 + d]).wait()

    def hot(values, row):
        return jnp.concatenate(
            [jnp.where(values == r, 1.0, 0.0).astype(jnp.bfloat16) for r in row], axis=1
        )

    def parts(values):
        return jnp.concatenate([in_three(v).astype(jnp.bfloat16) for v in values], axis=1)

    def slot_of(d):
        return [d * domains + k for k in range(domains)]

    def summed(d):
        return lax.dot_general(
            hot(halo_bc[...], [gather[q, 8:9, :] for q in slot_of(d)]),
            parts([gather[q, 0:8, :] for q in slot_of(d)]),
            NT, preferred_element_type=F32,
        )

    def owned(d):
        mine = (iota((blocks, blocks), 0) + me * blocks).astype(F32)
        values = [
            jnp.concatenate([gather[q, 0:8, :], gather_rest[q, 0:8, :]], axis=0) for q in slot_of(d)
        ]
        return lax.dot_general(
            parts(values), hot(mine, [gather_rest[q, 0:1, :] for q in slot_of(d)]),
            NT, preferred_element_type=F32,
        )

    arrived(2)
    stats = summed(2)
    arrived(0)
    stats = stats + summed(0)
    rest_arrived(0)
    table_sums = owned(0)
    arrived(1)
    rest_arrived(1)
    stats = stats + summed(1)
    table_sums = table_sums + owned(1)
    stats = stats[:, 0:8] + stats[:, 8:16] + stats[:, 16:24]
    wide = [jnp.broadcast_to(stats[:, k : k + 1], (blocks, 128)) for k in range(8)]
    heavy = 1.0 / jnp.maximum(wide[0], 1.0)
    drift = [wide[4 + c] * heavy for c in range(3)]
    spread = wide[7] * heavy - (drift[0] * drift[0] + drift[1] * drift[1] + drift[2] * drift[2])
    over = 1.0 / (3.0 * spread + EPSILON)
    centre = [wide[1 + c] * heavy - shift_bc[c] for c in range(3)]

    for i in range(blocks // 8):
        r = slice(8 * i, 8 * i + 8)
        alive = live_bc[r, :]
        for t in range(tiles):
            q = slice(128 * t, 128 * t + 128)
            mask = (lane + t * 128).astype(F32) < alive
            dv = [vel[c, r, q] - drift[c][r] for c in range(3)]
            dp = [pos[c, r, q] - centre[c][r] for c in range(3)]
            kin = (dv[0] * dv[0] + dv[1] * dv[1] + dv[2] * dv[2]) * over[r]
            rad = dp[0] * dp[0] + dp[1] * dp[1] + dp[2] * dp[2]
            kin_ref[r, q] = jnp.where(mask, kin, 0.0)
            rad_ref[r, q] = jnp.where(mask, rad, 0.0)

    own = table_sums[0:16] + table_sums[16:32] + table_sums[32:48]
    heavy = jnp.maximum(own[0:1], 1.0)
    c = [own[1 + i : 2 + i] / heavy for i in range(3)]
    d = [own[4 + i : 5 + i] / heavy for i in range(3)]
    spread = own[7:8] / heavy - (d[0] * d[0] + d[1] * d[1] + d[2] * d[2])
    spin = [
        own[9:10] / heavy - (c[1] * d[2] - c[2] * d[1]),
        own[10:11] / heavy - (c[2] * d[0] - c[0] * d[2]),
        own[11:12] / heavy - (c[0] * d[1] - c[1] * d[0]),
    ]

    table_ref[1:11, :] = jnp.concatenate([*c, *d, spread, *spin], axis=0)

    @pl.when(is_root)
    def _():
        sent = masses.at[pl.ds(0, n_roots - 1)]
        pltpu.make_async_copy(sent, sent, send_sem.at[0]).wait()

    @pl.when(jnp.logical_not(is_root))
    def _():
        sent = masses.at[pl.ds(0, n_roots)]
        pltpu.make_async_copy(sent, sent, send_sem.at[0]).wait()

    n_near = len(near)
    sent = gather.at[pl.ds(0, n_near), pl.ds(0, 9)]
    pltpu.make_async_copy(sent, sent, send_sem.at[1]).wait()
    sent = gather_rest.at[pl.ds(0, 2 * domains - 1), pl.ds(0, 4)]
    pltpu.make_async_copy(sent, sent, send_sem.at[3]).wait()

    def tell(there, a, k):
        return pltpu.make_async_remote_copy(
            line, line, send_sem.at[2], recv_sem.at[4],
            device_id=(there * planes_groups + a, k), device_id_type=MESH,
        )

    @pl.when(is_root)
    def _():
        others = masses.at[pl.ds(0, everyone - 1)]
        pltpu.make_async_copy(others, others, recv_sem.at[3]).wait()
        rows = masses[...].reshape(everyone // 8, 8, blocks)
        line[...] = jnp.sum(jnp.sum(rows, axis=0), axis=0, keepdims=True)

    for mine, (_, clients) in zip(i_am, tree):
        if clients:
            @pl.when(mine)
            def _():
                for client in clients:
                    tell(*client).start()

    @pl.when(jnp.logical_not(is_root))
    def _():
        pltpu.make_async_copy(line, line, recv_sem.at[4]).wait()

    table_ref[0:1, :] = own[0:1] * float(groups * domains * blocks) / line[...]

    for mine, (_, clients) in zip(i_am, tree):
        if clients:
            @pl.when(mine)
            def _():
                told = masses.at[pl.ds(0, len(clients))]
                pltpu.make_async_copy(told, told, send_sem.at[2]).wait()


def flush(table_ref, kin_ref, rad_ref, table_hbm, kin_hbm, rad_hbm, sem):
    pairs = ((kin_ref, kin_hbm), (rad_ref, rad_hbm), (table_ref, table_hbm))
    copies = [pltpu.make_async_copy(a, b, sem.at[i]) for i, (a, b) in enumerate(pairs)]
    for copy in copies:
        copy.start()
    for copy in copies:
        copy.wait()


def solution(mesh, plane_groups=PLANE_GROUPS):
    groups, domains = mesh.shape["grp"], mesh.shape["dom"]
    both = ("grp", "dom")

    def local(positions, velocities, masses, block_halo, block_shift, block_live, block_count, home_slot):
        blocks, width = masses.shape
        hbm = pl.BlockSpec(memory_space=pltpu.HBM)
        vmem = pl.BlockSpec(memory_space=pltpu.VMEM)
        long = home_slot.shape[0] // 128
        results = pl.pallas_call(
            functools.partial(kernel, (groups, domains, plane_groups)),
            out_shape=(
                pltpu.VMEM((11, blocks), F32),
                pltpu.VMEM((blocks, width), F32),
                pltpu.VMEM((blocks, width), F32),
            ),
            in_specs=[hbm] * 8,
            out_specs=(vmem, vmem, vmem),
            scratch_shapes=[
                pltpu.VMEM((3, blocks, width), F32),
                pltpu.VMEM((3, blocks, width), F32),
                pltpu.VMEM((blocks, width), F32),
                pltpu.VMEM((1, blocks), jnp.int32),
                pltpu.VMEM((3, blocks), jnp.int32),
                pltpu.VMEM((1, blocks), jnp.int32),
                pltpu.VMEM((1, 1), jnp.int32),
                pltpu.VMEM((long, 128), jnp.int32),
                pltpu.VMEM((blocks, blocks), F32),
                pltpu.VMEM((blocks, blocks), F32),
                pltpu.VMEM((3, blocks, blocks), F32),
                pltpu.VMEM((16, blocks), F32),
                pltpu.VMEM((8, blocks), F32),
                pltpu.VMEM((3 * domains, 16, blocks), F32),
                pltpu.VMEM((2 * domains, 8, blocks), F32),
                pltpu.VMEM((1, blocks), F32),
                pltpu.VMEM((groups * domains, blocks), F32),
                pltpu.VMEM((1, blocks), F32),
                pltpu.SemaphoreType.DMA((3 * CHUNKS,)),
                pltpu.SemaphoreType.DMA((4,)),
                pltpu.SemaphoreType.DMA,
                pltpu.SemaphoreType.DMA((4,)),
                pltpu.SemaphoreType.DMA((7,)),
            ],
            compiler_params=pltpu.CompilerParams(collective_id=0, has_side_effects=True),
        )(
            positions, velocities, masses,
            block_halo.reshape(1, blocks), block_shift, block_live.reshape(1, blocks), block_count.reshape(1, 1),
            home_slot.reshape(long, 128),
        )
        return pl.pallas_call(
            flush,
            out_shape=tuple(jax.ShapeDtypeStruct(r.shape, F32) for r in results),
            in_specs=[vmem] * 3,
            out_specs=(hbm,) * 3,
            scratch_shapes=[pltpu.SemaphoreType.DMA((3,))],
        )(*[pltpu.with_memory_space_constraint(r, pltpu.VMEM) for r in results])

    return jax.shard_map(
        local,
        mesh=mesh,
        in_specs=(
            P(None, both, None), P(None, both, None), P(both, None), P(both), P(None, both), P(both), P(both), P(),
        ),
        out_specs=(P(None, both), P(both, None), P(both, None)),
        check_vma=False,
    )
```

```python
import functools

import jax
import jax.numpy as jnp
from jax import lax
from jax.experimental import pallas as pl
from jax.experimental.pallas import tpu as pltpu
from jax.sharding import PartitionSpec as P

MESH = pl.DeviceIdType.MESH
EPSILON = 1e-6
PLANE_GROUPS = 4
ROOT = 1
CHUNKS = 4
F32 = jnp.float32
NT = (((1,), (1,)), ((), ()))


def wrapped(index, size):
    return jnp.where(index >= size, index - size, index)


def iota(shape, dim):
    return lax.broadcasted_iota(jnp.int32, shape, dim)


def in_three(x):
    high = x.astype(jnp.bfloat16).astype(F32)
    rest = x - high
    middle = rest.astype(jnp.bfloat16).astype(F32)
    return jnp.concatenate([high, middle, rest - middle], axis=0)


def roots_of(depth, planes_groups, domains):
    half = max(2, depth * 3 // 8)
    plane = [(a, k) for a in range(planes_groups) for k in range(domains)]
    tree = [((0, 0, 0), []), ((0, 0, ROOT), [])]
    if domains > 2:
        tree.append(((0, 0, 3), [(0, 0, k) for k in range(2, domains - 2) if k != 3]))
        tree.append(((0, 0, domains - 1), [(0, 0, domains - 2)]))
    tree += [((0, a, ROOT), [(0, a, k) for k in range(domains) if k != ROOT]) for a in range(1, planes_groups)]
    share = max(1, min(2, half - 1))
    for r in range(1, half):
        late = [p for p in range(half, depth) if half - 1 - (p - half) * share // (depth - half) == r]
        tree.append(((r, 0, ROOT), [(p, a, k) for p in [r] + late for a, k in plane if (p, a, k) != (r, 0, ROOT)]))
    return tree


def kernel(
    sizes,
    pos_hbm, vel_hbm, mass_hbm, halo_hbm, shift_hbm, live_hbm, count_hbm, slot_hbm,
    table_ref, kin_ref, rad_ref,
    pos, vel, mass, halo, shift, live, count, slots,
    live_bc, halo_bc, shift_bc, moments, rest, gather, gather_rest, mine_all, masses, line,
    in_sem, small_sem, count_sem, send_sem, recv_sem,
):
    groups, domains, planes_groups = sizes
    blocks = mass.shape[0]
    width = mass.shape[1]
    depth = groups // planes_groups
    g, j = lax.axis_index("grp"), lax.axis_index("dom")
    z = g // planes_groups
    x = g - z * planes_groups
    nxt = wrapped(g + 1, groups)
    prv = jnp.where(g == 0, groups - 1, g - 1)

    order = sorted(range(domains), key=lambda k: -min(k, domains - k))
    near = [(nxt, k, 0) for k in order] + [(prv, k, 2) for k in order] + [(g, k, 1) for k in order if k]
    me = g * domains + j
    everyone = groups * domains
    tree = roots_of(depth, planes_groups, domains)
    n_roots = len(tree)
    i_am = [(g == there * planes_groups + a) & (j == k) for (there, a, k), _ in tree]
    is_root = functools.reduce(jnp.logical_or, i_am)

    def domain(k):
        return wrapped(j + k, domains)

    def greet(grp, dom):
        pl.semaphore_signal(barrier, inc=1, device_id=(grp, dom), device_id_type=MESH)

    small = [
        pltpu.make_async_copy(live_hbm, live, small_sem.at[0]),
        pltpu.make_async_copy(count_hbm, count, count_sem),
        pltpu.make_async_copy(halo_hbm, halo, small_sem.at[1]),
        pltpu.make_async_copy(shift_hbm, shift, small_sem.at[2]),
        pltpu.make_async_copy(slot_hbm, slots, small_sem.at[3]),
    ]
    for copy in small[:2]:
        copy.start()
    part = blocks // CHUNKS
    big = []
    for c in range(CHUNKS):
        rows = pl.ds(c * part, part)
        big.append([
            pltpu.make_async_copy(mass_hbm.at[rows], mass.at[rows], in_sem.at[3 * c]),
            pltpu.make_async_copy(pos_hbm.at[:, rows], pos.at[:, rows], in_sem.at[3 * c + 1]),
            pltpu.make_async_copy(vel_hbm.at[:, rows], vel.at[:, rows], in_sem.at[3 * c + 2]),
        ])
        for copy in big[-1]:
            copy.start()

    for copy in small[2:]:
        copy.start()
    barrier = pltpu.get_barrier_semaphore()
    first, last = g == 0, x == planes_groups - 1

    @pl.when(x == 0)
    def _():
        for k in order:
            greet(prv, domain(k))

    @pl.when(jnp.logical_not(last) | (g != groups - 1))
    def _():
        for k in order:
            greet(nxt, domain(k))

    for k in order:
        if k:
            greet(g, domain(k))


    @pl.when(is_root)
    def _():
        @pl.loop(0, depth)
        def _(step):
            there = depth - 1 - step
            for a in range(planes_groups):
                for k in range(domains):
                    if (a, k) in {root[1:] for root, _ in tree}:
                        @pl.when((there * planes_groups + a != g) | (j != k))
                        def _():
                            greet(there * planes_groups + a, k)
                    else:
                        greet(there * planes_groups + a, k)

    for copy in small[:2]:
        copy.wait()

    row = iota((1, blocks), 1)
    live_row = jnp.where(row < count[...], live[...], 0).astype(F32)
    live_bc[...] = jnp.broadcast_to(live_row, (blocks, blocks)).T

    tiles = width // 128
    lane = iota((8, 128), 1)
    diagonal = lane - iota((8, 128), 0)

    def moment_step(i, sums):
        base = pl.multiple_of(i * 8, 8)
        rows = pl.ds(base, 8)
        alive = live_bc[rows, :]
        acc = None
        for t in range(tiles):
            cols = pl.ds(t * 128, 128)
            w = jnp.where((lane + t * 128).astype(F32) < alive, mass[rows, cols], 0.0)
            p = [pos[c, rows, cols] for c in range(3)]
            v = [vel[c, rows, cols] for c in range(3)]
            wv = [w * v[c] for c in range(3)]
            terms = [w] + [w * p[c] for c in range(3)] + wv
            terms.append(wv[0] * v[0] + wv[1] * v[1] + wv[2] * v[2])
            terms.append(p[1] * wv[2] - p[2] * wv[1])
            terms.append(p[2] * wv[0] - p[0] * wv[2])
            terms.append(p[0] * wv[1] - p[1] * wv[0])
            acc = terms if acc is None else [a + b for a, b in zip(acc, terms)]
        here = diagonal == base
        return tuple(
            s + jnp.where(here, jnp.sum(a, axis=1, keepdims=True), 0.0)
            for s, a in zip(sums, acc)
        )

    sums = tuple(jnp.zeros((8, 128), F32) for _ in range(11))
    for c in range(CHUNKS):
        for copy in big[c]:
            copy.wait()
        sums = lax.fori_loop(c * part // 8, (c + 1) * part // 8, moment_step, sums, unroll=4)
    for copy in small[2:]:
        copy.wait()
    halo_row = halo[...].astype(F32)
    shift_rows = shift[...].astype(F32)
    m = [jnp.sum(s, axis=0, keepdims=True) for s in sums]
    s = [shift_rows[c : c + 1] for c in range(3)]
    raw_p, mom_v = m[1:4], m[4:7]
    ang = [
        m[8] + (s[1] * mom_v[2] - s[2] * mom_v[1]),
        m[9] + (s[2] * mom_v[0] - s[0] * mom_v[2]),
        m[10] + (s[0] * mom_v[1] - s[1] * mom_v[0]),
    ]
    place = [raw_p[c] + s[c] * m[0] for c in range(3)]

    moments[0:9, :] = jnp.concatenate([m[0], *place, *mom_v, m[7], halo_row], axis=0)
    gather[domains + j, 0:9, :] = moments[0:9, :]
    whole = jnp.broadcast_to(jnp.sum(m[0], axis=1, keepdims=True), (1, blocks))
    mine_all[...] = whole
    masses[pl.ds(me, 1), :] = whole

    heard = jnp.where(first, 0, domains) + jnp.where(last, domains, 0) + jnp.where(is_root, n_roots - 1, n_roots)
    pl.semaphore_wait(barrier, domains - 1 + heard)

    for mine, ((there, a, k), _) in zip(i_am, tree):
        @pl.when(jnp.logical_not(mine))
        def _():
            pltpu.make_async_remote_copy(
                mine_all, masses.at[pl.ds(me, 1)], send_sem.at[0], recv_sem.at[3],
                device_id=(there * planes_groups + a, k), device_id_type=MESH,
            ).start()

    def send(d):
        for grp, k, kind in near:
            if kind == d:
                pltpu.make_async_remote_copy(
                    moments.at[pl.ds(0, 9)], gather.at[d * domains + j, pl.ds(0, 9)], send_sem.at[1], recv_sem.at[d],
                    device_id=(grp, domain(k)), device_id_type=MESH,
                ).start()

    def send_rest(d):
        for grp, k, kind in near:
            if kind == d:
                pltpu.make_async_remote_copy(
                    rest.at[pl.ds(0, 4)], gather_rest.at[d * domains + j, pl.ds(0, 4)], send_sem.at[3], recv_sem.at[5 + d],
                    device_id=(grp, domain(k)), device_id_type=MESH,
                ).start()

    @pl.when(last)
    def _():
        send(0)

    @pl.when(jnp.logical_not(first))
    def _():
        send(2)

    send(1)

    halo_int = halo[...]
    high_bits = halo_int // 128
    low_bits = halo_int - high_bits * 128
    table = slots[...]
    table_high = table // 256
    table_low = table - table_high * 256
    pick = jnp.where(iota((128, blocks), 0) == low_bits, 1.0, 0.0).astype(jnp.bfloat16)
    picked = jnp.dot(
        jnp.concatenate([table_high, table_low], axis=0).astype(F32).astype(jnp.bfloat16),
        pick,
        preferred_element_type=F32,
    )
    long = table.shape[0]
    both = picked[:long] * 256.0 + picked[long:]
    slot_row = jnp.sum(
        jnp.where(iota((long, blocks), 0) == high_bits, both, 0.0), axis=0, keepdims=True
    )

    rest[0:4, :] = jnp.concatenate([slot_row, *ang], axis=0)
    gather_rest[domains + j, 0:4, :] = rest[0:4, :]

    @pl.when(last)
    def _():
        send_rest(0)

    send_rest(1)

    halo_bc[...] = jnp.broadcast_to(halo_row, (blocks, blocks)).T
    for c in range(3):
        shift_bc[c] = jnp.broadcast_to(s[c], (blocks, blocks)).T

    def arrived(d):
        n = domains - 1 if d == 1 else domains
        span = gather.at[pl.ds(d * domains, n), pl.ds(0, 9)]
        pltpu.make_async_copy(span, span, recv_sem.at[d]).wait()

    def rest_arrived(d):
        n = domains - 1 if d == 1 else domains
        span = gather_rest.at[pl.ds(d * domains, n), pl.ds(0, 4)]
        pltpu.make_async_copy(span, span, recv_sem.at[5 + d]).wait()

    def hot(values, row):
        return jnp.concatenate(
            [jnp.where(values == r, 1.0, 0.0).astype(jnp.bfloat16) for r in row], axis=1
        )

    def parts(values):
        return jnp.concatenate([in_three(v).astype(jnp.bfloat16) for v in values], axis=1)

    def slot_of(d):
        return [d * domains + k for k in range(domains)]

    def summed(d):
        return lax.dot_general(
            hot(halo_bc[...], [gather[q, 8:9, :] for q in slot_of(d)]),
            parts([gather[q, 0:8, :] for q in slot_of(d)]),
            NT, preferred_element_type=F32,
        )

    def owned(d):
        mine = (iota((blocks, blocks), 0) + me * blocks).astype(F32)
        values = [
            jnp.concatenate([gather[q, 0:8, :], gather_rest[q, 0:8, :]], axis=0) for q in slot_of(d)
        ]
        return lax.dot_general(
            parts(values), hot(mine, [gather_rest[q, 0:1, :] for q in slot_of(d)]),
            NT, preferred_element_type=F32,
        )

    arrived(2)

    @pl.when(jnp.logical_not(last))
    def _():
        send(0)
        send_rest(0)

    stats = summed(2)
    arrived(1)
    rest_arrived(1)
    stats = stats + summed(1)
    table_sums = owned(1)
    arrived(0)

    @pl.when(first)
    def _():
        send(2)

    stats = stats + summed(0)
    stats = stats[:, 0:8] + stats[:, 8:16] + stats[:, 16:24]
    wide = [jnp.broadcast_to(stats[:, k : k + 1], (blocks, 128)) for k in range(8)]
    heavy = 1.0 / jnp.maximum(wide[0], 1.0)
    drift = [wide[4 + c] * heavy for c in range(3)]
    spread = wide[7] * heavy - (drift[0] * drift[0] + drift[1] * drift[1] + drift[2] * drift[2])
    over = 1.0 / (3.0 * spread + EPSILON)
    centre = [wide[1 + c] * heavy - shift_bc[c] for c in range(3)]

    for i in range(blocks // 8):
        r = slice(8 * i, 8 * i + 8)
        alive = live_bc[r, :]
        for t in range(tiles):
            q = slice(128 * t, 128 * t + 128)
            mask = (lane + t * 128).astype(F32) < alive
            dv = [vel[c, r, q] - drift[c][r] for c in range(3)]
            dp = [pos[c, r, q] - centre[c][r] for c in range(3)]
            kin = (dv[0] * dv[0] + dv[1] * dv[1] + dv[2] * dv[2]) * over[r]
            rad = dp[0] * dp[0] + dp[1] * dp[1] + dp[2] * dp[2]
            kin_ref[r, q] = jnp.where(mask, kin, 0.0)
            rad_ref[r, q] = jnp.where(mask, rad, 0.0)

    rest_arrived(0)
    table_sums = table_sums + owned(0)
    own = table_sums[0:16] + table_sums[16:32] + table_sums[32:48]
    heavy = jnp.maximum(own[0:1], 1.0)
    c = [own[1 + i : 2 + i] / heavy for i in range(3)]
    d = [own[4 + i : 5 + i] / heavy for i in range(3)]
    spread = own[7:8] / heavy - (d[0] * d[0] + d[1] * d[1] + d[2] * d[2])
    spin = [
        own[9:10] / heavy - (c[1] * d[2] - c[2] * d[1]),
        own[10:11] / heavy - (c[2] * d[0] - c[0] * d[2]),
        own[11:12] / heavy - (c[0] * d[1] - c[1] * d[0]),
    ]

    table_ref[1:11, :] = jnp.concatenate([*c, *d, spread, *spin], axis=0)

    @pl.when(is_root)
    def _():
        sent = masses.at[pl.ds(0, n_roots - 1)]
        pltpu.make_async_copy(sent, sent, send_sem.at[0]).wait()

    @pl.when(jnp.logical_not(is_root))
    def _():
        sent = masses.at[pl.ds(0, n_roots)]
        pltpu.make_async_copy(sent, sent, send_sem.at[0]).wait()

    n_near = len(near)
    sent = gather.at[pl.ds(0, n_near), pl.ds(0, 9)]
    pltpu.make_async_copy(sent, sent, send_sem.at[1]).wait()
    sent = gather_rest.at[pl.ds(0, 2 * domains - 1), pl.ds(0, 4)]
    pltpu.make_async_copy(sent, sent, send_sem.at[3]).wait()

    def tell(there, a, k):
        return pltpu.make_async_remote_copy(
            line, line, send_sem.at[2], recv_sem.at[4],
            device_id=(there * planes_groups + a, k), device_id_type=MESH,
        )

    @pl.when(is_root)
    def _():
        others = masses.at[pl.ds(0, everyone - 1)]
        pltpu.make_async_copy(others, others, recv_sem.at[3]).wait()
        rows = masses[...].reshape(everyone // 8, 8, blocks)
        line[...] = jnp.sum(jnp.sum(rows, axis=0), axis=0, keepdims=True)

    for mine, (_, clients) in zip(i_am, tree):
        if clients:
            @pl.when(mine)
            def _():
                for client in clients:
                    tell(*client).start()

    @pl.when(jnp.logical_not(is_root))
    def _():
        pltpu.make_async_copy(line, line, recv_sem.at[4]).wait()

    table_ref[0:1, :] = own[0:1] * float(groups * domains * blocks) / line[...]

    for mine, (_, clients) in zip(i_am, tree):
        if clients:
            @pl.when(mine)
            def _():
                told = masses.at[pl.ds(0, len(clients))]
                pltpu.make_async_copy(told, told, send_sem.at[2]).wait()


def flush(table_ref, kin_ref, rad_ref, table_hbm, kin_hbm, rad_hbm, sem):
    pairs = ((kin_ref, kin_hbm), (rad_ref, rad_hbm), (table_ref, table_hbm))
    copies = [pltpu.make_async_copy(a, b, sem.at[i]) for i, (a, b) in enumerate(pairs)]
    for copy in copies:
        copy.start()
    for copy in copies:
        copy.wait()


def solution(mesh, plane_groups=PLANE_GROUPS):
    groups, domains = mesh.shape["grp"], mesh.shape["dom"]
    both = ("grp", "dom")

    def local(positions, velocities, masses, block_halo, block_shift, block_live, block_count, home_slot):
        blocks, width = masses.shape
        hbm = pl.BlockSpec(memory_space=pltpu.HBM)
        vmem = pl.BlockSpec(memory_space=pltpu.VMEM)
        long = home_slot.shape[0] // 128
        results = pl.pallas_call(
            functools.partial(kernel, (groups, domains, plane_groups)),
            out_shape=(
                pltpu.VMEM((11, blocks), F32),
                pltpu.VMEM((blocks, width), F32),
                pltpu.VMEM((blocks, width), F32),
            ),
            in_specs=[hbm] * 8,
            out_specs=(vmem, vmem, vmem),
            scratch_shapes=[
                pltpu.VMEM((3, blocks, width), F32),
                pltpu.VMEM((3, blocks, width), F32),
                pltpu.VMEM((blocks, width), F32),
                pltpu.VMEM((1, blocks), jnp.int32),
                pltpu.VMEM((3, blocks), jnp.int32),
                pltpu.VMEM((1, blocks), jnp.int32),
                pltpu.VMEM((1, 1), jnp.int32),
                pltpu.VMEM((long, 128), jnp.int32),
                pltpu.VMEM((blocks, blocks), F32),
                pltpu.VMEM((blocks, blocks), F32),
                pltpu.VMEM((3, blocks, blocks), F32),
                pltpu.VMEM((16, blocks), F32),
                pltpu.VMEM((8, blocks), F32),
                pltpu.VMEM((3 * domains, 16, blocks), F32),
                pltpu.VMEM((2 * domains, 8, blocks), F32),
                pltpu.VMEM((1, blocks), F32),
                pltpu.VMEM((groups * domains, blocks), F32),
                pltpu.VMEM((1, blocks), F32),
                pltpu.SemaphoreType.DMA((3 * CHUNKS,)),
                pltpu.SemaphoreType.DMA((4,)),
                pltpu.SemaphoreType.DMA,
                pltpu.SemaphoreType.DMA((4,)),
                pltpu.SemaphoreType.DMA((7,)),
            ],
            compiler_params=pltpu.CompilerParams(collective_id=0, has_side_effects=True),
        )(
            positions, velocities, masses,
            block_halo.reshape(1, blocks), block_shift, block_live.reshape(1, blocks), block_count.reshape(1, 1),
            home_slot.reshape(long, 128),
        )
        return pl.pallas_call(
            flush,
            out_shape=tuple(jax.ShapeDtypeStruct(r.shape, F32) for r in results),
            in_specs=[vmem] * 3,
            out_specs=(hbm,) * 3,
            scratch_shapes=[pltpu.SemaphoreType.DMA((3,))],
        )(*[pltpu.with_memory_space_constraint(r, pltpu.VMEM) for r in results])

    return jax.shard_map(
        local,
        mesh=mesh,
        in_specs=(
            P(None, both, None), P(None, both, None), P(both, None), P(both), P(None, both), P(both), P(both), P(),
        ),
        out_specs=(P(None, both), P(both, None), P(both, None)),
        check_vma=False,
    )
```

```python
import functools

import jax
import jax.numpy as jnp
from jax import lax
from jax.experimental import pallas as pl
from jax.experimental.pallas import tpu as pltpu
from jax.sharding import PartitionSpec as P

MESH = pl.DeviceIdType.MESH
EPSILON = 1e-6
PLANE_GROUPS = 4
ROOT = 1
CHUNKS = 4
F32 = jnp.float32
NT = (((1,), (1,)), ((), ()))


def wrapped(index, size):
    return jnp.where(index >= size, index - size, index)


def iota(shape, dim):
    return lax.broadcasted_iota(jnp.int32, shape, dim)


def in_three(x):
    high = x.astype(jnp.bfloat16).astype(F32)
    rest = x - high
    middle = rest.astype(jnp.bfloat16).astype(F32)
    return jnp.concatenate([high, middle, rest - middle], axis=0)


def roots_of(depth, planes_groups, domains):
    half = max(2, depth * 3 // 8)
    plane = [(a, k) for a in range(planes_groups) for k in range(domains)]
    tree = [((0, 0, 0), []), ((0, 0, ROOT), [])]
    if domains > 2:
        tree.append(((0, 0, 3), [(0, 0, k) for k in range(2, domains - 2) if k != 3]))
        tree.append(((0, 0, domains - 1), [(0, 0, domains - 2)]))
    tree += [((0, a, ROOT), [(0, a, k) for k in range(domains) if k != ROOT]) for a in range(1, planes_groups)]
    share = max(1, min(2, half - 1))
    for r in range(1, half):
        late = [p for p in range(half, depth) if half - 1 - (p - half) * share // (depth - half) == r]
        tree.append(((r, 0, ROOT), [(p, a, k) for p in [r] + late for a, k in plane if (p, a, k) != (r, 0, ROOT)]))
    return tree


def kernel(
    sizes,
    pos_hbm, vel_hbm, mass_hbm, halo_hbm, shift_hbm, live_hbm, count_hbm, slot_hbm,
    table_ref, kin_ref, rad_ref,
    pos, vel, mass, halo, shift, live, count, slots,
    live_bc, halo_bc, shift_bc, moments, rest, gather, gather_rest, mine_all, masses, line,
    in_sem, small_sem, count_sem, send_sem, recv_sem,
):
    groups, domains, planes_groups = sizes
    blocks = mass.shape[0]
    width = mass.shape[1]
    depth = groups // planes_groups
    g, j = lax.axis_index("grp"), lax.axis_index("dom")
    z = g // planes_groups
    x = g - z * planes_groups
    nxt = wrapped(g + 1, groups)
    prv = jnp.where(g == 0, groups - 1, g - 1)

    order = sorted(range(domains), key=lambda k: -min(k, domains - k))
    near = [(nxt, k, 0) for k in order] + [(prv, k, 2) for k in order] + [(g, k, 1) for k in order if k]
    me = g * domains + j
    everyone = groups * domains
    tree = roots_of(depth, planes_groups, domains)
    n_roots = len(tree)
    i_am = [(g == there * planes_groups + a) & (j == k) for (there, a, k), _ in tree]
    is_root = functools.reduce(jnp.logical_or, i_am)

    def domain(k):
        return wrapped(j + k, domains)

    def greet(grp, dom):
        pl.semaphore_signal(barrier, inc=1, device_id=(grp, dom), device_id_type=MESH)

    small = [
        pltpu.make_async_copy(live_hbm, live, small_sem.at[0]),
        pltpu.make_async_copy(count_hbm, count, count_sem),
        pltpu.make_async_copy(halo_hbm, halo, small_sem.at[1]),
        pltpu.make_async_copy(shift_hbm, shift, small_sem.at[2]),
        pltpu.make_async_copy(slot_hbm, slots, small_sem.at[3]),
    ]
    for copy in small[:2]:
        copy.start()
    part = blocks // CHUNKS
    big = []
    for c in range(CHUNKS):
        rows = pl.ds(c * part, part)
        big.append([
            pltpu.make_async_copy(mass_hbm.at[rows], mass.at[rows], in_sem.at[3 * c]),
            pltpu.make_async_copy(pos_hbm.at[:, rows], pos.at[:, rows], in_sem.at[3 * c + 1]),
            pltpu.make_async_copy(vel_hbm.at[:, rows], vel.at[:, rows], in_sem.at[3 * c + 2]),
        ])
        for copy in big[-1]:
            copy.start()

    for copy in small[2:]:
        copy.start()
    barrier = pltpu.get_barrier_semaphore()
    first, last = g == 0, x == planes_groups - 1

    for k in order:
        if k:
            greet(g, domain(k))

    @pl.when(x == 0)
    def _():
        for k in order:
            greet(prv, domain(k))

    @pl.when(jnp.logical_not(last) | (g != groups - 1))
    def _():
        for k in order:
            greet(nxt, domain(k))


    @pl.when(is_root)
    def _():
        @pl.loop(0, depth)
        def _(step):
            there = depth - 1 - step
            for a in range(planes_groups):
                for k in range(domains):
                    if (a, k) in {root[1:] for root, _ in tree}:
                        @pl.when((there * planes_groups + a != g) | (j != k))
                        def _():
                            greet(there * planes_groups + a, k)
                    else:
                        greet(there * planes_groups + a, k)

    for copy in small[:2]:
        copy.wait()

    row = iota((1, blocks), 1)
    live_row = jnp.where(row < count[...], live[...], 0).astype(F32)
    live_bc[...] = jnp.broadcast_to(live_row, (blocks, blocks)).T

    tiles = width // 128
    lane = iota((8, 128), 1)
    diagonal = lane - iota((8, 128), 0)

    def moment_step(i, sums):
        base = pl.multiple_of(i * 8, 8)
        rows = pl.ds(base, 8)
        alive = live_bc[rows, :]
        acc = None
        for t in range(tiles):
            cols = pl.ds(t * 128, 128)
            w = jnp.where((lane + t * 128).astype(F32) < alive, mass[rows, cols], 0.0)
            p = [pos[c, rows, cols] for c in range(3)]
            v = [vel[c, rows, cols] for c in range(3)]
            wv = [w * v[c] for c in range(3)]
            terms = [w] + [w * p[c] for c in range(3)] + wv
            terms.append(wv[0] * v[0] + wv[1] * v[1] + wv[2] * v[2])
            terms.append(p[1] * wv[2] - p[2] * wv[1])
            terms.append(p[2] * wv[0] - p[0] * wv[2])
            terms.append(p[0] * wv[1] - p[1] * wv[0])
            acc = terms if acc is None else [a + b for a, b in zip(acc, terms)]
        here = diagonal == base
        return tuple(
            s + jnp.where(here, jnp.sum(a, axis=1, keepdims=True), 0.0)
            for s, a in zip(sums, acc)
        )

    sums = tuple(jnp.zeros((8, 128), F32) for _ in range(11))
    for c in range(CHUNKS):
        for copy in big[c]:
            copy.wait()
        sums = lax.fori_loop(c * part // 8, (c + 1) * part // 8, moment_step, sums, unroll=4)
    for copy in small[2:]:
        copy.wait()
    halo_row = halo[...].astype(F32)
    shift_rows = shift[...].astype(F32)
    m = [jnp.sum(s, axis=0, keepdims=True) for s in sums]
    s = [shift_rows[c : c + 1] for c in range(3)]
    raw_p, mom_v = m[1:4], m[4:7]
    ang = [
        m[8] + (s[1] * mom_v[2] - s[2] * mom_v[1]),
        m[9] + (s[2] * mom_v[0] - s[0] * mom_v[2]),
        m[10] + (s[0] * mom_v[1] - s[1] * mom_v[0]),
    ]
    place = [raw_p[c] + s[c] * m[0] for c in range(3)]

    moments[0:9, :] = jnp.concatenate([m[0], *place, *mom_v, m[7], halo_row], axis=0)
    gather[domains + j, 0:9, :] = moments[0:9, :]
    whole = jnp.broadcast_to(jnp.sum(m[0], axis=1, keepdims=True), (1, blocks))
    mine_all[...] = whole
    masses[pl.ds(me, 1), :] = whole

    heard = jnp.where(first, 0, domains) + jnp.where(last, domains, 0) + jnp.where(is_root, n_roots - 1, n_roots)
    pl.semaphore_wait(barrier, domains - 1 + heard)

    for mine, ((there, a, k), _) in zip(i_am, tree):
        @pl.when(jnp.logical_not(mine))
        def _():
            pltpu.make_async_remote_copy(
                mine_all, masses.at[pl.ds(me, 1)], send_sem.at[0], recv_sem.at[3],
                device_id=(there * planes_groups + a, k), device_id_type=MESH,
            ).start()

    def send(d):
        for grp, k, kind in near:
            if kind == d:
                pltpu.make_async_remote_copy(
                    moments.at[pl.ds(0, 9)], gather.at[d * domains + j, pl.ds(0, 9)], send_sem.at[1], recv_sem.at[d],
                    device_id=(grp, domain(k)), device_id_type=MESH,
                ).start()

    def send_rest(d):
        for grp, k, kind in near:
            if kind == d:
                pltpu.make_async_remote_copy(
                    rest.at[pl.ds(0, 4)], gather_rest.at[d * domains + j, pl.ds(0, 4)], send_sem.at[3], recv_sem.at[5 + d],
                    device_id=(grp, domain(k)), device_id_type=MESH,
                ).start()

    @pl.when(last)
    def _():
        send(0)

    @pl.when(jnp.logical_not(first))
    def _():
        send(2)

    send(1)

    halo_int = halo[...]
    high_bits = halo_int // 128
    low_bits = halo_int - high_bits * 128
    table = slots[...]
    table_high = table // 256
    table_low = table - table_high * 256
    pick = jnp.where(iota((128, blocks), 0) == low_bits, 1.0, 0.0).astype(jnp.bfloat16)
    picked = jnp.dot(
        jnp.concatenate([table_high, table_low], axis=0).astype(F32).astype(jnp.bfloat16),
        pick,
        preferred_element_type=F32,
    )
    long = table.shape[0]
    both = picked[:long] * 256.0 + picked[long:]
    slot_row = jnp.sum(
        jnp.where(iota((long, blocks), 0) == high_bits, both, 0.0), axis=0, keepdims=True
    )

    rest[0:4, :] = jnp.concatenate([slot_row, *ang], axis=0)
    gather_rest[domains + j, 0:4, :] = rest[0:4, :]

    @pl.when(last)
    def _():
        send_rest(0)

    send_rest(1)

    halo_bc[...] = jnp.broadcast_to(halo_row, (blocks, blocks)).T
    for c in range(3):
        shift_bc[c] = jnp.broadcast_to(s[c], (blocks, blocks)).T

    def arrived(d):
        n = domains - 1 if d == 1 else domains
        span = gather.at[pl.ds(d * domains, n), pl.ds(0, 9)]
        pltpu.make_async_copy(span, span, recv_sem.at[d]).wait()

    def rest_arrived(d):
        n = domains - 1 if d == 1 else domains
        span = gather_rest.at[pl.ds(d * domains, n), pl.ds(0, 4)]
        pltpu.make_async_copy(span, span, recv_sem.at[5 + d]).wait()

    def hot(values, row):
        return jnp.concatenate(
            [jnp.where(values == r, 1.0, 0.0).astype(jnp.bfloat16) for r in row], axis=1
        )

    def parts(values):
        return jnp.concatenate([in_three(v).astype(jnp.bfloat16) for v in values], axis=1)

    def slot_of(d):
        return [d * domains + k for k in range(domains)]

    def summed(d):
        return lax.dot_general(
            hot(halo_bc[...], [gather[q, 8:9, :] for q in slot_of(d)]),
            parts([gather[q, 0:8, :] for q in slot_of(d)]),
            NT, preferred_element_type=F32,
        )

    def owned(d):
        mine = (iota((blocks, blocks), 0) + me * blocks).astype(F32)
        values = [
            jnp.concatenate([gather[q, 0:8, :], gather_rest[q, 0:8, :]], axis=0) for q in slot_of(d)
        ]
        return lax.dot_general(
            parts(values), hot(mine, [gather_rest[q, 0:1, :] for q in slot_of(d)]),
            NT, preferred_element_type=F32,
        )

    arrived(2)

    @pl.when(jnp.logical_not(last))
    def _():
        send(0)
        send_rest(0)

    stats = summed(2)
    arrived(1)
    rest_arrived(1)
    stats = stats + summed(1)
    table_sums = owned(1)
    arrived(0)

    @pl.when(first)
    def _():
        send(2)

    stats = stats + summed(0)
    stats = stats[:, 0:8] + stats[:, 8:16] + stats[:, 16:24]
    wide = [jnp.broadcast_to(stats[:, k : k + 1], (blocks, 128)) for k in range(8)]
    heavy = 1.0 / jnp.maximum(wide[0], 1.0)
    drift = [wide[4 + c] * heavy for c in range(3)]
    spread = wide[7] * heavy - (drift[0] * drift[0] + drift[1] * drift[1] + drift[2] * drift[2])
    over = 1.0 / (3.0 * spread + EPSILON)
    centre = [wide[1 + c] * heavy - shift_bc[c] for c in range(3)]

    for i in range(blocks // 8):
        r = slice(8 * i, 8 * i + 8)
        alive = live_bc[r, :]
        for t in range(tiles):
            q = slice(128 * t, 128 * t + 128)
            mask = (lane + t * 128).astype(F32) < alive
            dv = [vel[c, r, q] - drift[c][r] for c in range(3)]
            dp = [pos[c, r, q] - centre[c][r] for c in range(3)]
            kin = (dv[0] * dv[0] + dv[1] * dv[1] + dv[2] * dv[2]) * over[r]
            rad = dp[0] * dp[0] + dp[1] * dp[1] + dp[2] * dp[2]
            kin_ref[r, q] = jnp.where(mask, kin, 0.0)
            rad_ref[r, q] = jnp.where(mask, rad, 0.0)

    rest_arrived(0)
    table_sums = table_sums + owned(0)
    own = table_sums[0:16] + table_sums[16:32] + table_sums[32:48]
    heavy = jnp.maximum(own[0:1], 1.0)
    c = [own[1 + i : 2 + i] / heavy for i in range(3)]
    d = [own[4 + i : 5 + i] / heavy for i in range(3)]
    spread = own[7:8] / heavy - (d[0] * d[0] + d[1] * d[1] + d[2] * d[2])
    spin = [
        own[9:10] / heavy - (c[1] * d[2] - c[2] * d[1]),
        own[10:11] / heavy - (c[2] * d[0] - c[0] * d[2]),
        own[11:12] / heavy - (c[0] * d[1] - c[1] * d[0]),
    ]

    table_ref[1:11, :] = jnp.concatenate([*c, *d, spread, *spin], axis=0)

    @pl.when(is_root)
    def _():
        sent = masses.at[pl.ds(0, n_roots - 1)]
        pltpu.make_async_copy(sent, sent, send_sem.at[0]).wait()

    @pl.when(jnp.logical_not(is_root))
    def _():
        sent = masses.at[pl.ds(0, n_roots)]
        pltpu.make_async_copy(sent, sent, send_sem.at[0]).wait()

    n_near = len(near)
    sent = gather.at[pl.ds(0, n_near), pl.ds(0, 9)]
    pltpu.make_async_copy(sent, sent, send_sem.at[1]).wait()
    sent = gather_rest.at[pl.ds(0, 2 * domains - 1), pl.ds(0, 4)]
    pltpu.make_async_copy(sent, sent, send_sem.at[3]).wait()

    def tell(there, a, k):
        return pltpu.make_async_remote_copy(
            line, line, send_sem.at[2], recv_sem.at[4],
            device_id=(there * planes_groups + a, k), device_id_type=MESH,
        )

    @pl.when(is_root)
    def _():
        others = masses.at[pl.ds(0, everyone - 1)]
        pltpu.make_async_copy(others, others, recv_sem.at[3]).wait()
        rows = masses[...].reshape(everyone // 8, 8, blocks)
        line[...] = jnp.sum(jnp.sum(rows, axis=0), axis=0, keepdims=True)

    for mine, (_, clients) in zip(i_am, tree):
        if clients:
            @pl.when(mine)
            def _():
                for client in clients:
                    tell(*client).start()

    @pl.when(jnp.logical_not(is_root))
    def _():
        pltpu.make_async_copy(line, line, recv_sem.at[4]).wait()

    table_ref[0:1, :] = own[0:1] * float(groups * domains * blocks) / line[...]

    for mine, (_, clients) in zip(i_am, tree):
        if clients:
            @pl.when(mine)
            def _():
                told = masses.at[pl.ds(0, len(clients))]
                pltpu.make_async_copy(told, told, send_sem.at[2]).wait()


def flush(table_ref, kin_ref, rad_ref, table_hbm, kin_hbm, rad_hbm, sem):
    pairs = ((kin_ref, kin_hbm), (rad_ref, rad_hbm), (table_ref, table_hbm))
    copies = [pltpu.make_async_copy(a, b, sem.at[i]) for i, (a, b) in enumerate(pairs)]
    for copy in copies:
        copy.start()
    for copy in copies:
        copy.wait()


def solution(mesh, plane_groups=PLANE_GROUPS):
    groups, domains = mesh.shape["grp"], mesh.shape["dom"]
    both = ("grp", "dom")

    def local(positions, velocities, masses, block_halo, block_shift, block_live, block_count, home_slot):
        blocks, width = masses.shape
        hbm = pl.BlockSpec(memory_space=pltpu.HBM)
        vmem = pl.BlockSpec(memory_space=pltpu.VMEM)
        long = home_slot.shape[0] // 128
        results = pl.pallas_call(
            functools.partial(kernel, (groups, domains, plane_groups)),
            out_shape=(
                pltpu.VMEM((11, blocks), F32),
                pltpu.VMEM((blocks, width), F32),
                pltpu.VMEM((blocks, width), F32),
            ),
            in_specs=[hbm] * 8,
            out_specs=(vmem, vmem, vmem),
            scratch_shapes=[
                pltpu.VMEM((3, blocks, width), F32),
                pltpu.VMEM((3, blocks, width), F32),
                pltpu.VMEM((blocks, width), F32),
                pltpu.VMEM((1, blocks), jnp.int32),
                pltpu.VMEM((3, blocks), jnp.int32),
                pltpu.VMEM((1, blocks), jnp.int32),
                pltpu.VMEM((1, 1), jnp.int32),
                pltpu.VMEM((long, 128), jnp.int32),
                pltpu.VMEM((blocks, blocks), F32),
                pltpu.VMEM((blocks, blocks), F32),
                pltpu.VMEM((3, blocks, blocks), F32),
                pltpu.VMEM((16, blocks), F32),
                pltpu.VMEM((8, blocks), F32),
                pltpu.VMEM((3 * domains, 16, blocks), F32),
                pltpu.VMEM((2 * domains, 8, blocks), F32),
                pltpu.VMEM((1, blocks), F32),
                pltpu.VMEM((groups * domains, blocks), F32),
                pltpu.VMEM((1, blocks), F32),
                pltpu.SemaphoreType.DMA((3 * CHUNKS,)),
                pltpu.SemaphoreType.DMA((4,)),
                pltpu.SemaphoreType.DMA,
                pltpu.SemaphoreType.DMA((4,)),
                pltpu.SemaphoreType.DMA((7,)),
            ],
            compiler_params=pltpu.CompilerParams(collective_id=0, has_side_effects=True),
        )(
            positions, velocities, masses,
            block_halo.reshape(1, blocks), block_shift, block_live.reshape(1, blocks), block_count.reshape(1, 1),
            home_slot.reshape(long, 128),
        )
        return pl.pallas_call(
            flush,
            out_shape=tuple(jax.ShapeDtypeStruct(r.shape, F32) for r in results),
            in_specs=[vmem] * 3,
            out_specs=(hbm,) * 3,
            scratch_shapes=[pltpu.SemaphoreType.DMA((3,))],
        )(*[pltpu.with_memory_space_constraint(r, pltpu.VMEM) for r in results])

    return jax.shard_map(
        local,
        mesh=mesh,
        in_specs=(
            P(None, both, None), P(None, both, None), P(both, None), P(both), P(None, both), P(both), P(both), P(),
        ),
        out_specs=(P(None, both), P(both, None), P(both, None)),
        check_vma=False,
    )
```
